32 devices in a mesh: gx: 2 (over core), gy: 2 (over x), gz: 8 (over z, y).
Axes of the slice: x: 2, y: 2, z: 4, core: 2. Of those that a mesh axis runs over, the one named last changes fastest.
Arguments:
- old_pos: float32 [3, 32768], P(None, ('gx', 'gy', 'gz')), may hold values from -6 to 6
- new_pos: float32 [3, 32768], P(None, ('gx', 'gy', 'gz')), may hold values from -6 to 6
- inv_mass: float32 [32768], P(('gx', 'gy', 'gz')), may hold values from 0.05 to 1
- rest_length: float32 [32768], P(('gx', 'gy', 'gz')), may hold values from 0.8 to 1.6
- bond_pairs: int32 [2, 32768], P(None, ('gx', 'gy', 'gz')), may hold values from 0 to 1311, as said below
- live: int32 [32768], P(('gx', 'gy', 'gz')), may hold values from 0 to 1, as said below
- send_index: int32 [192, 48], P(('gx', 'gy', 'gz')), may hold values from 0 to 1023, as said below
Outputs:
- displacement: float32 [3, 32768], P(None, ('gx', 'gy', 'gz'))
- multipliers: float32 [32768], P(('gx', 'gy', 'gz'))
The draws below stay inside these ranges and needn't reach their ends.
Inputs may be any that keep to these rules, and one draw needn't show every extreme that they name: `bond_pairs`: in domain k's slots, row 0 is an own atom (0 to 1023). Row 1 indexes the domain's extended list: its own atoms, then six blocks of 48 received atoms, block 2a + s holding, in order, list 2a + s of the neighbour one step down (s = 0) or up (s = 1) along axis a. Every atom is in at most two live constraints, each received atom is the second atom of at most one live constraint, and exactly 216 live constraints of each domain name a received atom. `live`: padding slots change nothing. `send_index`: rows 6k to 6k + 5 are domain k's lists of own atoms; list 2a + s goes to the neighbour one step up (s = 0) or down (s = 1) along axis a, periodically. The 288 entries of a domain are distinct.
All inputs are finite; a program needn't handle non-finite values.
Results may differ from the reference program's by a relative error of at most 0.0001.
Values sent between devices are 32-bit elements; how exact they have to be, the bound alone decides.
A program may use at most 64 MiB of HBM per device.

```python
import math
import jax
import jax.numpy as jnp
from jax import lax

ATOMS_DEV = 1024
HALO_ROWS = 48
CHAIN_HEADS = 384
CROSS_BONDS = 216
ORDER = 4
DOMAINS = 32
ATOMS = 32768
N_GX = 2
N_GY = 2
N_GZ = 8


def one_domain(key):
    keys = jax.random.split(key, 6)
    position = jnp.arange(ATOMS_DEV, dtype=jnp.int32)
    atom_slot = jax.random.permutation(keys[0], ATOMS_DEV).astype(jnp.int32)
    ranking = jax.random.permutation(keys[1], ATOMS_DEV).astype(jnp.int32)
    heading = (ranking < CHAIN_HEADS) | (position == 0)
    ending = jnp.concatenate([heading[1:], jnp.ones((1,), dtype=bool)])
    tiebreak = jax.random.permutation(keys[2], ATOMS_DEV).astype(jnp.int32)
    end_score = ending.astype(jnp.int32) * (1 << 24) + tiebreak
    unused_end, cross_pos = lax.top_k(end_score, CROSS_BONDS)
    halo_slot = jax.random.permutation(keys[3], 6 * HALO_ROWS).astype(jnp.int32)[:CROSS_BONDS] + ATOMS_DEV
    following = jnp.roll(atom_slot, -1)
    second_atom = jnp.where(ending, 0, following).astype(jnp.int32)
    second_atom = second_atom.at[cross_pos].set(halo_slot)
    alive = jnp.where(ending, 0, 1).astype(jnp.int32).at[cross_pos].set(1)
    ordering = jax.random.permutation(keys[4], ATOMS_DEV).astype(jnp.int32)
    first_atom = atom_slot[ordering]
    second_atom = second_atom[ordering]
    alive = alive[ordering]
    head_tie = jax.random.permutation(keys[5], ATOMS_DEV).astype(jnp.int32)
    head_score = heading.astype(jnp.int32) * (1 << 24) + head_tie
    unused_head, head_pos = lax.top_k(head_score, 6 * HALO_ROWS)
    sending = atom_slot[head_pos].reshape(6, HALO_ROWS)
    return (first_atom, second_atom, alive, sending)


def all_domains(key):
    numbers = jnp.arange(DOMAINS, dtype=jnp.int32)
    domain_keys = jax.vmap(lambda number: jax.random.fold_in(key, number))(numbers)
    return jax.vmap(one_domain)(domain_keys)


def draw_bond_pairs(key, part):
    first_atom, second_atom, alive, sending = all_domains(key)
    return jnp.stack([first_atom.reshape(-1), second_atom.reshape(-1)], 0).astype(jnp.int32)


def draw_live(key, part):
    first_atom, second_atom, alive, sending = all_domains(key)
    return alive.reshape(-1).astype(jnp.int32)


def draw_send_index(key, part):
    first_atom, second_atom, alive, sending = all_domains(key)
    return sending.reshape(DOMAINS * 6, HALO_ROWS).astype(jnp.int32)


def block_levels(stream_key, dims, cuts, low, high):
    def one(dim, parts):
        draws = jax.random.uniform(jax.random.fold_in(jax.random.fold_in(stream_key, 6), dim), (parts,), jnp.float32, low / len(cuts), high / len(cuts))
        return jnp.repeat(jnp.exp(draws), dims[dim] // parts).reshape((-1,) + (1,) * (len(dims) - dim - 1))

    level = one(*cuts[0])
    for cut in cuts[1:]:
        level = level * one(*cut)
    return level


def normal_values(key, dims, scale, most, cuts=(), kind=jnp.bfloat16):
    drawn = scale * jax.random.normal(key, dims, jnp.float32)
    if cuts:
        drawn = drawn * block_levels(key, dims, cuts, -0.22, 0.18)
    return jnp.clip(drawn, -most, most).astype(kind)


def setup_inputs(seed: int = 0) -> dict:
    streams_of = jax.random.split(jax.random.key(seed), 8)
    return {
        "old_pos": normal_values(streams_of[0], (3, ATOMS), 1.0, 6.0, ((1, 32),), jnp.float32),
        "new_pos": normal_values(streams_of[1], (3, ATOMS), 1.0, 6.0, ((1, 32),), jnp.float32),
        "inv_mass": jnp.clip(jnp.exp(math.log(1.0) - 2.9957323 * jax.random.uniform(streams_of[2], (ATOMS,), jnp.float32) ** block_levels(streams_of[2], (ATOMS,), ((0, 32),), -0.2, 0.2)), 0.05, 1.0),
        "rest_length": jnp.clip(0.8 + 0.8 * jax.random.uniform(streams_of[3], (ATOMS,), jnp.float32) ** block_levels(streams_of[3], (ATOMS,), ((0, 32),), -0.2, 0.2), 0.8, 1.6),
        "bond_pairs": draw_bond_pairs(jax.random.fold_in(streams_of[7], 71), 0),
        "live": draw_live(jax.random.fold_in(streams_of[7], 71), 0),
        "send_index": draw_send_index(jax.random.fold_in(streams_of[7], 71), 0),
    }


def owners(bond_pairs, send_index):
    slot_index = jnp.arange(ATOMS, dtype=jnp.int32)
    domain = slot_index // ATOMS_DEV
    first_atom = domain * ATOMS_DEV + bond_pairs[0].astype(jnp.int32)
    local_second = bond_pairs[1].astype(jnp.int32)
    remote = local_second >= ATOMS_DEV
    offset = jnp.maximum(local_second - ATOMS_DEV, 0)
    block = offset // HALO_ROWS
    row_index = offset % HALO_ROWS
    coord_x = domain // (N_GY * N_GZ)
    coord_y = domain // N_GZ % N_GY
    coord_z = domain % N_GZ
    stride = jnp.where(block % 2 == 0, -1, 1)
    axis_pick = block // 2
    source_x = (coord_x + jnp.where(axis_pick == 0, stride, 0)) % N_GX
    source_y = (coord_y + jnp.where(axis_pick == 1, stride, 0)) % N_GY
    source_z = (coord_z + jnp.where(axis_pick == 2, stride, 0)) % N_GZ
    source = (source_x * N_GY + source_y) * N_GZ + source_z
    sent_atom = send_index[source * 6 + block, row_index].astype(jnp.int32)
    second_atom = jnp.where(remote, source * ATOMS_DEV + sent_atom, domain * ATOMS_DEV + local_second)
    return (first_atom, second_atom)

def reference(old_pos, new_pos, inv_mass, rest_length, bond_pairs, live, send_index):
    first_atom, second_atom = owners(bond_pairs, send_index)

    def across_bond(field):
        return field[:, first_atom] - field[:, second_atom]
    old_span = across_bond(old_pos)
    unit_dir = old_span / jnp.sqrt(lax.optimization_barrier(jnp.sum(old_span * old_span, 0)) + 0.25)
    scaling = live.astype(jnp.float32) / jnp.sqrt(inv_mass[first_atom] + inv_mass[second_atom])

    def atom_shift(values):
        contrib = unit_dir * (scaling * values)[None]
        blank = jnp.zeros((3, ATOMS), jnp.float32)
        summed = blank.at[:, first_atom].add(contrib).at[:, second_atom].add(-contrib)
        return inv_mass[None] * summed

    def coupling(values):
        return values - scaling * lax.optimization_barrier(jnp.sum(unit_dir * across_bond(atom_shift(values)), 0))

    def expansion(start):
        series = start
        current = start
        for repeat in range(ORDER):
            current = coupling(current)
            series = series + current
        return series
    right_side = scaling * (lax.optimization_barrier(jnp.sum(unit_dir * across_bond(new_pos), 0)) - rest_length)
    first_sol = expansion(right_side)
    shifted_pos = new_pos - atom_shift(first_sol)
    stretch = across_bond(shifted_pos)
    length_sq = lax.optimization_barrier(jnp.sum(stretch * stretch, 0))
    floor_sq = 0.25 * rest_length * rest_length
    target = jnp.sqrt(jnp.maximum(2.0 * rest_length * rest_length - length_sq, floor_sq))
    second_sol = expansion(scaling * (rest_length - target))
    final_pos = shifted_pos - atom_shift(second_sol)
    return (final_pos - new_pos, first_sol + second_sol)
```

```python
import functools

import jax
import jax.numpy as jnp
from jax import lax
from jax.experimental import pallas as pl
from jax.experimental.pallas import tpu as pltpu
from jax.sharding import PartitionSpec as P

ORDER = 4
AXES = ("gx", "gy", "gz")
LANES = 128
HALF = 64
ROUNDS = 2 * ORDER + 3
BIG = 4


class Pick:
    def __init__(self, row, lane, count):
        self.lane = lane & (LANES - 1)
        self.masks = [row == r for r in range(count)]

    def __call__(self, table, start=0, init=None, stop=None):
        out = jnp.zeros(self.lane.shape, table.dtype) if init is None else init
        count = table.shape[0] if stop is None else stop
        for r in range(count):
            line = jnp.broadcast_to(table[r : r + 1, :], self.lane.shape)
            found = jnp.take_along_axis(line, self.lane, axis=1, mode="promise_in_bounds")
            out = jnp.where(self.masks[start + r], found, out)
        return out


def to_row(x):
    return jnp.concatenate([x[r : r + 1, :] for r in range(x.shape[0])], axis=1)


def to_rows(x):
    return jnp.concatenate(
        [x[:, LANES * r : LANES * (r + 1)] for r in range(x.shape[1] // LANES)], axis=0
    )


def one_hot_lanes(lane_row):
    shape = (LANES, lane_row.shape[1])
    hit = lax.broadcasted_iota(jnp.int32, shape, 0) == lane_row
    return jnp.where(hit, 1.0, 0.0).astype(jnp.bfloat16)


def place(row_row, values, hot, rows):
    shape = (rows, row_row.shape[1])
    hit = lax.broadcasted_iota(jnp.int32, shape, 0) == row_row
    left = jnp.concatenate([jnp.where(hit, v.astype(jnp.float32), 0.0) for v in values], axis=0)
    out = lax.dot_general(
        left.astype(jnp.bfloat16), hot, (((1,), (1,)), ((), ())), preferred_element_type=jnp.float32
    ).astype(jnp.int32)
    return [out[rows * i : rows * (i + 1)] for i in range(len(values))]


def kernel(sizes, width, old_ref, new_ref, mass_ref, rest_ref, pairs_ref, live_ref, send_ref,
           move_ref, mult_ref, listed, out_big, in_big, out_small, in_small, send_sem, recv_sem):
    rows = mass_ref.shape[0]
    slots = rows * LANES

    slot_of = {}
    targets = []
    for a, axis in enumerate(AXES):
        me, count = lax.axis_index(axis), sizes[a]
        up, down = lax.rem(me + 1, count), lax.rem(me + count - 1, count)
        base = len(targets)
        if count == 2:
            slot_of[a] = (base, base)
            targets.append(({axis: up}, base))
        else:
            slot_of[a] = (base, base + 1)
            targets.append(({axis: up}, base))
            targets.append(({axis: down}, base + 1))

    barrier = pltpu.get_barrier_semaphore()
    for device, unused in targets:
        pl.semaphore_signal(barrier, inc=1, device_id=device, device_id_type=pl.DeviceIdType.MESH)

    started = []

    def launch(number, tiles):
        if number < 2:
            for i, tile in enumerate(tiles):
                out_big[number, i] = tile
        else:
            out_small[number - 2] = tiles[0]
        copies = []
        for n, (device, landing) in enumerate(targets):
            copies.append(
                pltpu.make_async_remote_copy(
                    src_ref=out_big.at[number] if number < 2 else out_small.at[number - 2],
                    dst_ref=in_big.at[number, landing] if number < 2 else in_small.at[number - 2, landing],
                    send_sem=send_sem.at[number, n],
                    recv_sem=recv_sem.at[number, landing],
                    device_id=device,
                    device_id_type=pl.DeviceIdType.MESH,
                )
            )
        for copy in copies:
            copy.start()
        started.extend(copies)
        return copies

    tile_row = lax.broadcasted_iota(jnp.int32, (8, LANES), 0)
    tile_lane = lax.broadcasted_iota(jnp.int32, (8, LANES), 1)
    back_half = tile_lane >= HALF

    def arrived(number, copies, index, both_out=False):
        tiles = [
            in_big[number, n, index] if number < 2 else in_small[number - 2, n]
            for n in range(len(targets))
        ]
        out = tiles[slot_of[0][0]]
        for a in range(3):
            low, high = slot_of[a]
            if low == high:
                out = jnp.where(tile_row // 2 == a, tiles[low], out)
                continue
            odd = tile_row % 2 == 1
            from_up = odd if both_out else odd != back_half
            out = jnp.where(tile_row // 2 == a, jnp.where(from_up, tiles[high], tiles[low]), out)
        return out

    def wait(copies):
        for copy in copies:
            copy.wait_recv()

    listed[...] = jnp.zeros_like(listed)
    listed[0:6, 0:width] = send_ref[...]
    listed[0:6, HALF : HALF + width] = send_ref[...]
    sending = listed[...]
    at_listed = Pick(sending >> 7, sending, rows)

    old = [to_rows(old_ref[c : c + 1, :]) for c in range(3)]
    new = [to_rows(new_ref[c : c + 1, :]) for c in range(3)]
    mass = mass_ref[...]
    fields = old + new + [mass]
    picked = [at_listed(f) for f in fields]
    picked.append(picked[6])
    tiles = [jnp.where(back_half, picked[2 * i + 1], picked[2 * i]) for i in range(BIG)]
    pl.semaphore_wait(barrier, len(targets))
    copies = launch(0, tiles)

    first = to_rows(pairs_ref[0:1, :])
    second = to_rows(pairs_ref[1:2, :])
    live = live_ref[...]
    own = second < slots
    offset = jnp.maximum(second - slots, 0)
    block = jnp.zeros_like(offset)
    for i in range(1, 6):
        block = block + jnp.where(offset >= width * i, 1, 0)
    second_row = jnp.where(own, second >> 7, rows + block)
    second_lane = jnp.where(own, second & (LANES - 1), offset - width * block)
    at_first = Pick(first >> 7, first, rows)
    at_second = Pick(second_row, second_lane, rows + 6)
    number = (
        lax.broadcasted_iota(jnp.int32, (rows, LANES), 0) * LANES
        + lax.broadcasted_iota(jnp.int32, (rows, LANES), 1)
        + 1
    )
    counted = (live != 0) & (first != second)

    def code_row(mask_first, mask_second):
        return jnp.concatenate(
            [to_row(jnp.where(mask_first, first >> 7, -1)), to_row(jnp.where(mask_second, second_row, -1))], 1
        )

    hot = one_hot_lanes(jnp.concatenate([pairs_ref[0:1, :] & (LANES - 1), to_row(second_lane)], 1))
    number_row = to_row(number)
    number_row = jnp.concatenate([number_row, number_row + slots], 1)
    parts = [number_row >> 6, number_row & 63]
    high, low = place(code_row(counted, counted), parts, hot, rows + 8)
    ends = high * 64 + low
    ends_own = ends[:rows]
    ends_halo = ends[rows:]

    listed_row = jnp.concatenate([sending[b : b + 1, :] for b in range(6)], axis=1)
    spot = lax.broadcasted_iota(jnp.int32, listed_row.shape, 1)
    spot_block = spot // LANES
    spot_lane = spot % LANES
    place_block, place_lane = place(
        jnp.where(spot_lane < width, listed_row >> 7, -1),
        [spot_block + 1, spot_lane],
        one_hot_lanes(listed_row & (LANES - 1)),
        rows,
    )

    def split(code):
        minus = code > slots
        index = jnp.where(minus, code - slots, code) - 1
        return jnp.where(code > 0, index >> 7, -1), index & (LANES - 1), jnp.where(minus, -1.0, 1.0)

    other_first = jnp.where(counted, at_first(ends_own) - number, 0)
    other_second = jnp.where(counted & own, at_second(ends_own) - (number + slots), 0)

    def partner(other, at, remote_row=None, remote_lane=None):
        row, lane, sign = split(other)
        there = at(place_block)
        far_row = jnp.where(there > 0, rows + there - 1, -1)
        far_lane = HALF + at(place_lane)
        if remote_row is not None:
            far_row = jnp.where(own, far_row, remote_row)
            far_lane = jnp.where(own, far_lane, remote_lane)
        near = other > 0
        return (
            Pick(jnp.where(near, row, far_row), jnp.where(near, lane, far_lane), rows + 6),
            jnp.where(near, sign, 1.0),
        )

    along_first, sign_first = partner(other_first, at_first)
    along_second, sign_second = partner(other_second, at_second, second_row, second_lane)

    send_code = jnp.where(back_half, pltpu.roll(ends_halo, HALF, 1), at_listed(ends_own))
    send_row, send_lane, send_sign = split(send_code)
    to_send = Pick(send_row, send_lane, rows)

    lead_first = counted & ((other_first <= 0) | (number < other_first))
    lead_second = counted & own & ((other_second <= 0) | (number + slots < other_second))
    high, low = place(code_row(lead_first, lead_second), parts, hot, rows)
    lead = high * 64 + low
    row, lane, lead_sign = split(lead)
    at_lead = Pick(row, lane, rows)
    row, lane, rest_sign = split(ends_own - lead)
    at_rest = Pick(row, lane, rows)
    at_far = Pick(jnp.where(place_block > 0, place_block - 1, -1), HALF + place_lane, 6)

    near_first = [at_first(f) for f in fields]
    near_second = [at_second(f) for f in fields]

    wait(copies)
    got = [arrived(0, copies, i, both_out=True) for i in range(BIG)]
    got_back = [pltpu.roll(t, HALF, 1) for t in got[:3]]
    halo = [got[0], got_back[0], got[1], got_back[1], got[2], got_back[2], got[3]]
    near_second = [at_second(h, rows, g, 6) for h, g in zip(halo, near_second)]
    mass_first, mass_second = near_first[6], near_second[6]
    old_span = [near_first[c] - near_second[c] for c in range(3)]
    new_span = [near_first[3 + c] - near_second[3 + c] for c in range(3)]
    dot = lambda p, q: p[0] * q[0] + p[1] * q[1] + p[2] * q[2]
    norm = jnp.sqrt(dot(old_span, old_span) + 0.25)
    unit = [s / norm for s in old_span]
    mass_sum = mass_first + mass_second
    scaling = live.astype(jnp.float32) / jnp.sqrt(mass_sum)
    rest = rest_ref[...]
    weight = [scaling * u for u in unit]
    x = scaling * (dot(unit, new_span) - rest)

    copies = launch(1, [send_sign * to_send(w) for w in weight] + [to_send(x)])
    diagonal = 1.0 - dot(weight, weight) * mass_sum
    pair_first = [along_first(w) for w in weight]
    pair_second = [along_second(w) for w in weight]
    lead_weight = [lead_sign * at_lead(w) for w in weight]
    rest_weight = [rest_sign * at_rest(w) for w in weight]
    near = along_first(x), along_second(x)
    wait(copies)
    got = [arrived(1, copies, i) for i in range(BIG)]
    pair_first = [sign_first * along_first(h, rows, p, 6) for h, p in zip(got[:3], pair_first)]
    pair_second = [sign_second * along_second(h, rows, p, 6) for h, p in zip(got[:3], pair_second)]
    far_weight = [at_far(h, stop=6) for h in got[:3]]
    factor_first = -mass_first * dot(weight, pair_first)
    factor_second = mass_second * dot(weight, pair_second)
    halo_x = got[3]

    def finish(near, halo_x):
        return along_first(halo_x, rows, near[0], 6), along_second(halo_x, rows, near[1], 6)

    def expand(x, halo_x, near, number):
        total_x, total_halo = x, halo_x
        g = finish(near, halo_x)
        total_g = list(g)
        for step in range(ORDER):
            x = diagonal * x + factor_first * g[0] + factor_second * g[1]
            copies = launch(number, [to_send(x)])
            total_x = total_x + x
            near = along_first(x), along_second(x)
            wait(copies)
            halo_x = arrived(number, copies, 0)
            g = finish(near, halo_x)
            total_g = [t + h for t, h in zip(total_g, g)]
            total_halo = total_halo + halo_x
            number += 1
        return total_x, total_halo, total_g

    first_sol, first_halo, first_g = expand(x, halo_x, near, 2)
    move_g = mass_first * first_g[0], mass_second * first_g[1]
    move_x = mass_sum * first_sol
    stretch = [
        new_span[c] - move_x * weight[c] - move_g[0] * pair_first[c] + move_g[1] * pair_second[c]
        for c in range(3)
    ]
    length_sq = dot(stretch, stretch)
    target = jnp.sqrt(jnp.maximum(2.0 * rest * rest - length_sq, 0.25 * rest * rest))
    y = scaling * (rest - target)
    copies = launch(2 + ORDER, [to_send(y)])
    near = along_first(y), along_second(y)
    wait(copies)
    second_sol, second_halo, unused = expand(y, arrived(2 + ORDER, copies, 0), near, 3 + ORDER)

    total = first_sol + second_sol
    mult_ref[...] = total
    at_ends = at_lead(total), at_rest(total), at_far(first_halo + second_halo, stop=6)
    for c in range(3):
        moved = -mass * (
            lead_weight[c] * at_ends[0] + rest_weight[c] * at_ends[1] + far_weight[c] * at_ends[2]
        )
        move_ref[c : c + 1, :] = to_row(moved)
    for copy in started:
        copy.wait_send()


def solution(mesh):
    sizes = tuple(mesh.shape[a] for a in AXES)

    def per_device(old_pos, new_pos, inv_mass, rest_length, bond_pairs, live, send_index):
        atoms = old_pos.shape[1]
        rows = atoms // LANES
        width = send_index.shape[1]
        links = sum(1 if n == 2 else 2 for n in sizes)
        tall = lambda v: v.reshape(rows, LANES)
        vmem = pl.BlockSpec(memory_space=pltpu.VMEM)
        tile = (8, LANES)
        moved, mult = pl.pallas_call(
            functools.partial(kernel, sizes, width),
            out_shape=(
                jax.ShapeDtypeStruct((3, atoms), jnp.float32),
                jax.ShapeDtypeStruct((rows, LANES), jnp.float32),
            ),
            in_specs=[vmem] * 7,
            out_specs=(vmem, vmem),
            scratch_shapes=[
                pltpu.VMEM(tile, jnp.int32),
                pltpu.VMEM((2, BIG) + tile, jnp.float32),
                pltpu.VMEM((2, links, BIG) + tile, jnp.float32),
                pltpu.VMEM((ROUNDS - 2,) + tile, jnp.float32),
                pltpu.VMEM((ROUNDS - 2, links) + tile, jnp.float32),
                pltpu.SemaphoreType.DMA((ROUNDS, links)),
                pltpu.SemaphoreType.DMA((ROUNDS, links)),
            ],
            compiler_params=pltpu.CompilerParams(collective_id=0, has_side_effects=True),
        )(old_pos, new_pos, tall(inv_mass), tall(rest_length), bond_pairs, tall(live), send_index)
        return moved, mult.reshape(atoms)

    spread = P(AXES)
    wide = P(None, AXES)
    return jax.shard_map(
        per_device,
        mesh=mesh,
        in_specs=(wide, wide, spread, spread, wide, spread, P(AXES, None)),
        out_specs=(wide, spread),
        check_vma=False,
    )
```

```python
import functools

import jax
import jax.numpy as jnp
from jax import lax
from jax.experimental import pallas as pl
from jax.experimental.pallas import tpu as pltpu
from jax.sharding import PartitionSpec as P

ORDER = 4
AXES = ("gx", "gy", "gz")
LANES = 128
HALF = 64
ROUNDS = 2 * ORDER + 3
BIG = 4


class Plan:
    def __init__(self, sizes, start, turn, flip):
        self.sizes, self.start, self.turn, self.flip = sizes, start, turn, flip

    def site_of(self, domain):
        ix, iy, iz = domain
        nx, ny, nz = self.sizes
        spot = (self.start + self.turn * iz) % nz
        if nz % 2 == 0:
            late = spot // (nz // 2)
            spot = (1 - late) * 2 * spot + late * (2 * (nz - 1 - spot) + 1)
        return [(ix + iy + iz + self.flip) % nx, iy, spot]

    def domain_on(self, site):
        core, iy, spot = site
        nx, ny, nz = self.sizes
        if nz % 2 == 0:
            line, side = spot // 2, spot % 2
            spot = (1 - side) * line + side * (nz - 1 - line)
        iz = (self.turn * (spot - self.start + nz) + nz) % nz
        return [(core + 2 * nx * (ny + nz) - iy - iz - self.flip) % nx, iy, iz]

    def named(self, site):
        return dict(zip(AXES, site))

    def price(self):
        worst = total = 0
        for ix in range(self.sizes[0]):
            for iy in range(self.sizes[1]):
                for iz in range(self.sizes[2]):
                    site = self.site_of((ix, iy, iz))
                    assert tuple(self.domain_on(site)) == (ix, iy, iz)
                    if tuple(site) == (ix, iy, iz):
                        return None
                    hops = abs(site[2] // 2 - iz // 2) + abs(site[2] % 2 - iz % 2)
                    worst, total = max(worst, hops), total + hops
        return worst, total


def best_plan(sizes):
    plans = [
        Plan(sizes, start, turn, flip)
        for start in range(sizes[2])
        for turn in (1, sizes[2] - 1)
        for flip in range(sizes[0])
    ]
    priced = [(p.price(), i) for i, p in enumerate(plans)]
    return plans[min(p for p in priced if p[0] is not None)[1]]


class Pick:
    def __init__(self, row, lane, count):
        self.lane = lane & (LANES - 1)
        self.masks = [row == r for r in range(count)]

    def __call__(self, table, start=0, init=None, stop=None):
        out = jnp.zeros(self.lane.shape, table.dtype) if init is None else init
        count = table.shape[0] if stop is None else stop
        for r in range(count):
            line = jnp.broadcast_to(table[r : r + 1, :], self.lane.shape)
            found = jnp.take_along_axis(line, self.lane, axis=1, mode="promise_in_bounds")
            out = jnp.where(self.masks[start + r], found, out)
        return out


def to_row(x):
    return jnp.concatenate([x[r : r + 1, :] for r in range(x.shape[0])], axis=1)


def to_rows(x):
    return jnp.concatenate(
        [x[:, LANES * r : LANES * (r + 1)] for r in range(x.shape[1] // LANES)], axis=0
    )


def one_hot_lanes(lane_row):
    shape = (LANES, lane_row.shape[1])
    hit = lax.broadcasted_iota(jnp.int32, shape, 0) == lane_row
    return jnp.where(hit, 1.0, 0.0).astype(jnp.bfloat16)


def place(row_row, values, hot, rows):
    shape = (rows, row_row.shape[1])
    hit = lax.broadcasted_iota(jnp.int32, shape, 0) == row_row
    left = jnp.concatenate([jnp.where(hit, v.astype(jnp.float32), 0.0) for v in values], axis=0)
    out = lax.dot_general(
        left.astype(jnp.bfloat16), hot, (((1,), (1,)), ((), ())), preferred_element_type=jnp.float32
    ).astype(jnp.int32)
    return [out[rows * i : rows * (i + 1)] for i in range(len(values))]


def kernel(plan, width, *refs):
    home, results, away, own_results = refs[0:7], refs[7:9], refs[9:16], refs[16:18]
    listed, out_big, in_big, out_small, in_small, send_sem, recv_sem, carry_sem = refs[18:]
    move_ref, mult_ref = own_results
    sizes = plan.sizes
    rows = home[2].shape[0]
    slots = rows * LANES

    here = [lax.axis_index(axis) for axis in AXES]
    domain = plan.domain_on(here)
    sites = [plan.site_of(here), domain]

    slot_of = {}
    targets = []
    for a in range(3):
        moved_by = lambda step: plan.site_of(
            [(v + (step if i == a else 0)) % n for i, (v, n) in enumerate(zip(domain, sizes))]
        )
        base = len(targets)
        up = plan.named(moved_by(1))
        if sizes[a] == 2:
            slot_of[a] = (base, base)
            targets.append((up, base))
        else:
            slot_of[a] = (base, base + 1)
            targets.append((up, base))
            targets.append((plan.named(moved_by(sizes[a] - 1)), base + 1))

    mesh_ids = pl.DeviceIdType.MESH
    barrier = pltpu.get_barrier_semaphore()
    greeted = [plan.named(site) for site in sites] + [device for device, unused in targets]
    for device in greeted:
        pl.semaphore_signal(barrier, inc=1, device_id=device, device_id_type=mesh_ids)
    pl.semaphore_wait(barrier, len(greeted))

    def carry(sources, ends, device, base):
        copies = [
            pltpu.make_async_remote_copy(
                src_ref=source,
                dst_ref=end,
                send_sem=carry_sem.at[0, base + i],
                recv_sem=carry_sem.at[1, base + i],
                device_id=device,
                device_id_type=mesh_ids,
            )
            for i, (source, end) in enumerate(zip(sources, ends))
        ]
        for copy in copies:
            copy.start()
        return copies

    inward = carry(home, away, greeted[0], 0)
    for copy in inward:
        copy.wait_recv()
    old_ref, new_ref, mass_ref, rest_ref, pairs_ref, live_ref, send_ref = away

    started = []

    def launch(number, tiles):
        if number < 2:
            for i, tile in enumerate(tiles):
                out_big[number, i] = tile
        else:
            out_small[number - 2] = tiles[0]
        copies = []
        for n, (device, landing) in enumerate(targets):
            copies.append(
                pltpu.make_async_remote_copy(
                    src_ref=out_big.at[number] if number < 2 else out_small.at[number - 2],
                    dst_ref=in_big.at[number, landing] if number < 2 else in_small.at[number - 2, landing],
                    send_sem=send_sem.at[number, n],
                    recv_sem=recv_sem.at[number, landing],
                    device_id=device,
                    device_id_type=mesh_ids,
                )
            )
        for copy in copies:
            copy.start()
        started.extend(copies)
        return copies

    tile_row = lax.broadcasted_iota(jnp.int32, (8, LANES), 0)
    tile_lane = lax.broadcasted_iota(jnp.int32, (8, LANES), 1)
    back_half = tile_lane >= HALF

    def arrived(number, copies, index, both_out=False):
        tiles = [
            in_big[number, n, index] if number < 2 else in_small[number - 2, n]
            for n in range(len(targets))
        ]
        out = tiles[slot_of[0][0]]
        for a in range(3):
            low, high = slot_of[a]
            if low == high:
                out = jnp.where(tile_row // 2 == a, tiles[low], out)
                continue
            odd = tile_row % 2 == 1
            from_up = odd if both_out else odd != back_half
            out = jnp.where(tile_row // 2 == a, jnp.where(from_up, tiles[high], tiles[low]), out)
        return out

    def wait(copies):
        for copy in copies:
            copy.wait_recv()

    listed[...] = jnp.zeros_like(listed)
    listed[0:6, 0:width] = send_ref[...]
    listed[0:6, HALF : HALF + width] = send_ref[...]
    sending = listed[...]
    at_listed = Pick(sending >> 7, sending, rows)

    old = [to_rows(old_ref[c : c + 1, :]) for c in range(3)]
    new = [to_rows(new_ref[c : c + 1, :]) for c in range(3)]
    mass = mass_ref[...]
    fields = old + new + [mass]
    picked = [at_listed(f) for f in fields]
    picked.append(picked[6])
    tiles = [jnp.where(back_half, picked[2 * i + 1], picked[2 * i]) for i in range(BIG)]
    copies = launch(0, tiles)

    first = to_rows(pairs_ref[0:1, :])
    second = to_rows(pairs_ref[1:2, :])
    live = live_ref[...]
    own = second < slots
    offset = jnp.maximum(second - slots, 0)
    block = jnp.zeros_like(offset)
    for i in range(1, 6):
        block = block + jnp.where(offset >= width * i, 1, 0)
    second_row = jnp.where(own, second >> 7, rows + block)
    second_lane = jnp.where(own, second & (LANES - 1), offset - width * block)
    at_first = Pick(first >> 7, first, rows)
    at_second = Pick(second_row, second_lane, rows + 6)
    number = (
        lax.broadcasted_iota(jnp.int32, (rows, LANES), 0) * LANES
        + lax.broadcasted_iota(jnp.int32, (rows, LANES), 1)
        + 1
    )
    counted = (live != 0) & (first != second)

    def code_row(mask_first, mask_second):
        return jnp.concatenate(
            [to_row(jnp.where(mask_first, first >> 7, -1)), to_row(jnp.where(mask_second, second_row, -1))], 1
        )

    hot = one_hot_lanes(jnp.concatenate([pairs_ref[0:1, :] & (LANES - 1), to_row(second_lane)], 1))
    number_row = to_row(number)
    number_row = jnp.concatenate([number_row, number_row + slots], 1)
    parts = [number_row >> 6, number_row & 63]
    high, low = place(code_row(counted, counted), parts, hot, rows + 8)
    ends = high * 64 + low
    ends_own = ends[:rows]
    ends_halo = ends[rows:]

    listed_row = jnp.concatenate([sending[b : b + 1, :] for b in range(6)], axis=1)
    spot = lax.broadcasted_iota(jnp.int32, listed_row.shape, 1)
    spot_block = spot // LANES
    spot_lane = spot % LANES
    place_block, place_lane = place(
        jnp.where(spot_lane < width, listed_row >> 7, -1),
        [spot_block + 1, spot_lane],
        one_hot_lanes(listed_row & (LANES - 1)),
        rows,
    )

    def split(code):
        minus = code > slots
        index = jnp.where(minus, code - slots, code) - 1
        return jnp.where(code > 0, index >> 7, -1), index & (LANES - 1), jnp.where(minus, -1.0, 1.0)

    other_first = jnp.where(counted, at_first(ends_own) - number, 0)
    other_second = jnp.where(counted & own, at_second(ends_own) - (number + slots), 0)

    def partner(other, at, remote_row=None, remote_lane=None):
        row, lane, sign = split(other)
        there = at(place_block)
        far_row = jnp.where(there > 0, rows + there - 1, -1)
        far_lane = HALF + at(place_lane)
        if remote_row is not None:
            far_row = jnp.where(own, far_row, remote_row)
            far_lane = jnp.where(own, far_lane, remote_lane)
        near = other > 0
        return (
            Pick(jnp.where(near, row, far_row), jnp.where(near, lane, far_lane), rows + 6),
            jnp.where(near, sign, 1.0),
        )

    along_first, sign_first = partner(other_first, at_first)
    along_second, sign_second = partner(other_second, at_second, second_row, second_lane)

    send_code = jnp.where(back_half, pltpu.roll(ends_halo, HALF, 1), at_listed(ends_own))
    send_row, send_lane, send_sign = split(send_code)
    to_send = Pick(send_row, send_lane, rows)

    lead_first = counted & ((other_first <= 0) | (number < other_first))
    lead_second = counted & own & ((other_second <= 0) | (number + slots < other_second))
    high, low = place(code_row(lead_first, lead_second), parts, hot, rows)
    lead = high * 64 + low
    row, lane, lead_sign = split(lead)
    at_lead = Pick(row, lane, rows)
    row, lane, rest_sign = split(ends_own - lead)
    at_rest = Pick(row, lane, rows)
    at_far = Pick(jnp.where(place_block > 0, place_block - 1, -1), HALF + place_lane, 6)

    near_first = [at_first(f) for f in fields]
    near_second = [at_second(f) for f in fields]

    wait(copies)
    got = [arrived(0, copies, i, both_out=True) for i in range(BIG)]
    got_back = [pltpu.roll(t, HALF, 1) for t in got[:3]]
    halo = [got[0], got_back[0], got[1], got_back[1], got[2], got_back[2], got[3]]
    near_second = [at_second(h, rows, g, 6) for h, g in zip(halo, near_second)]
    mass_first, mass_second = near_first[6], near_second[6]
    old_span = [near_first[c] - near_second[c] for c in range(3)]
    new_span = [near_first[3 + c] - near_second[3 + c] for c in range(3)]
    dot = lambda p, q: p[0] * q[0] + p[1] * q[1] + p[2] * q[2]
    norm = jnp.sqrt(dot(old_span, old_span) + 0.25)
    unit = [s / norm for s in old_span]
    mass_sum = mass_first + mass_second
    scaling = live.astype(jnp.float32) / jnp.sqrt(mass_sum)
    rest = rest_ref[...]
    weight = [scaling * u for u in unit]
    x = scaling * (dot(unit, new_span) - rest)

    copies = launch(1, [send_sign * to_send(w) for w in weight] + [to_send(x)])
    diagonal = 1.0 - dot(weight, weight) * mass_sum
    pair_first = [along_first(w) for w in weight]
    pair_second = [along_second(w) for w in weight]
    lead_weight = [lead_sign * at_lead(w) for w in weight]
    rest_weight = [rest_sign * at_rest(w) for w in weight]
    near = along_first(x), along_second(x)
    wait(copies)
    got = [arrived(1, copies, i) for i in range(BIG)]
    pair_first = [sign_first * along_first(h, rows, p, 6) for h, p in zip(got[:3], pair_first)]
    pair_second = [sign_second * along_second(h, rows, p, 6) for h, p in zip(got[:3], pair_second)]
    far_weight = [at_far(h, stop=6) for h in got[:3]]
    factor_first = -mass_first * dot(weight, pair_first)
    factor_second = mass_second * dot(weight, pair_second)
    halo_x = got[3]

    def finish(near, halo_x):
        return along_first(halo_x, rows, near[0], 6), along_second(halo_x, rows, near[1], 6)

    def expand(x, halo_x, near, number):
        total_x, total_halo = x, halo_x
        g = finish(near, halo_x)
        total_g = list(g)
        for step in range(ORDER):
            x = diagonal * x + factor_first * g[0] + factor_second * g[1]
            copies = launch(number, [to_send(x)])
            total_x = total_x + x
            near = along_first(x), along_second(x)
            wait(copies)
            halo_x = arrived(number, copies, 0)
            g = finish(near, halo_x)
            total_g = [t + h for t, h in zip(total_g, g)]
            total_halo = total_halo + halo_x
            number += 1
        return total_x, total_halo, total_g

    first_sol, first_halo, first_g = expand(x, halo_x, near, 2)
    move_g = mass_first * first_g[0], mass_second * first_g[1]
    move_x = mass_sum * first_sol
    stretch = [
        new_span[c] - move_x * weight[c] - move_g[0] * pair_first[c] + move_g[1] * pair_second[c]
        for c in range(3)
    ]
    length_sq = dot(stretch, stretch)
    target = jnp.sqrt(jnp.maximum(2.0 * rest * rest - length_sq, 0.25 * rest * rest))
    y = scaling * (rest - target)
    copies = launch(2 + ORDER, [to_send(y)])
    near = along_first(y), along_second(y)
    wait(copies)
    second_sol, second_halo, unused = expand(y, arrived(2 + ORDER, copies, 0), near, 3 + ORDER)

    total = first_sol + second_sol
    mult_ref[...] = total
    at_ends = at_lead(total), at_rest(total), at_far(first_halo + second_halo, stop=6)
    for c in range(3):
        moved = -mass * (
            lead_weight[c] * at_ends[0] + rest_weight[c] * at_ends[1] + far_weight[c] * at_ends[2]
        )
        move_ref[c : c + 1, :] = to_row(moved)
    outward = carry(own_results, results, greeted[1], len(home))
    for copy in started + inward + outward:
        copy.wait_send()
    for copy in outward:
        copy.wait_recv()


def solution(mesh):
    sizes = tuple(mesh.shape[a] for a in AXES)
    plan = best_plan(sizes)

    def per_device(old_pos, new_pos, inv_mass, rest_length, bond_pairs, live, send_index):
        atoms = old_pos.shape[1]
        rows = atoms // LANES
        width = send_index.shape[1]
        links = sum(1 if n == 2 else 2 for n in sizes)
        tall = lambda v: v.reshape(rows, LANES)
        vmem = pl.BlockSpec(memory_space=pltpu.VMEM)
        tile = (8, LANES)
        moved, mult = pl.pallas_call(
            functools.partial(kernel, plan, width),
            out_shape=(
                jax.ShapeDtypeStruct((3, atoms), jnp.float32),
                jax.ShapeDtypeStruct((rows, LANES), jnp.float32),
            ),
            in_specs=[vmem] * 7,
            out_specs=(vmem, vmem),
            scratch_shapes=[
                pltpu.VMEM((3, atoms), jnp.float32),
                pltpu.VMEM((3, atoms), jnp.float32),
                pltpu.VMEM((rows, LANES), jnp.float32),
                pltpu.VMEM((rows, LANES), jnp.float32),
                pltpu.VMEM((2, atoms), jnp.int32),
                pltpu.VMEM((rows, LANES), jnp.int32),
                pltpu.VMEM(send_index.shape, jnp.int32),
                pltpu.VMEM((3, atoms), jnp.float32),
                pltpu.VMEM((rows, LANES), jnp.float32),
                pltpu.VMEM(tile, jnp.int32),
                pltpu.VMEM((2, BIG) + tile, jnp.float32),
                pltpu.VMEM((2, links, BIG) + tile, jnp.float32),
                pltpu.VMEM((ROUNDS - 2,) + tile, jnp.float32),
                pltpu.VMEM((ROUNDS - 2, links) + tile, jnp.float32),
                pltpu.SemaphoreType.DMA((ROUNDS, links)),
                pltpu.SemaphoreType.DMA((ROUNDS, links)),
                pltpu.SemaphoreType.DMA((2, 9)),
            ],
            compiler_params=pltpu.CompilerParams(collective_id=0, has_side_effects=True),
        )(old_pos, new_pos, tall(inv_mass), tall(rest_length), bond_pairs, tall(live), send_index)
        return moved, mult.reshape(atoms)

    spread = P(AXES)
    wide = P(None, AXES)
    return jax.shard_map(
        per_device,
        mesh=mesh,
        in_specs=(wide, wide, spread, spread, wide, spread, P(AXES, None)),
        out_specs=(wide, spread),
        check_vma=False,
    )
```

```python
import functools

import jax
import jax.numpy as jnp
from jax import lax
from jax.experimental import pallas as pl
from jax.experimental.pallas import tpu as pltpu
from jax.sharding import PartitionSpec as P

ORDER = 4
AXES = ("gx", "gy", "gz")
LANES = 128
HALF = 64
ROUNDS = 2 * ORDER + 3
BIG = 4


class Plan:
    def __init__(self, sizes, start, turn, flip):
        self.sizes, self.start, self.turn, self.flip = sizes, start, turn, flip

    def site_of(self, domain):
        ix, iy, iz = domain
        nx, ny, nz = self.sizes
        spot = (self.start + self.turn * iz) % nz
        if nz % 2 == 0:
            late = spot // (nz // 2)
            spot = (1 - late) * 2 * spot + late * (2 * (nz - 1 - spot) + 1)
        return [(ix + iy + iz + self.flip) % nx, iy, spot]

    def domain_on(self, site):
        core, iy, spot = site
        nx, ny, nz = self.sizes
        if nz % 2 == 0:
            line, side = spot // 2, spot % 2
            spot = (1 - side) * line + side * (nz - 1 - line)
        iz = (self.turn * (spot - self.start + nz) + nz) % nz
        return [(core + 2 * nx * (ny + nz) - iy - iz - self.flip) % nx, iy, iz]

    def named(self, site):
        return dict(zip(AXES, site))

    def around(self, domain):
        found = []
        for a, n in enumerate(self.sizes):
            for step in (1,) if n == 2 else (1, n - 1):
                found.append([(v + step) % n if i == a else v for i, v in enumerate(domain)])
        return found

    def price(self):
        worst = total = 0
        for ix in range(self.sizes[0]):
            for iy in range(self.sizes[1]):
                for iz in range(self.sizes[2]):
                    assert self.domain_on(self.site_of((ix, iy, iz))) == [ix, iy, iz]
                    for domain in [(ix, iy, iz)] + self.around((ix, iy, iz)):
                        site = self.site_of(domain)
                        hops = abs(site[2] // 2 - iz // 2) + abs(site[2] % 2 - iz % 2)
                        hops += abs(site[1] - iy)
                        worst, total = max(worst, hops), total + hops
        return worst, total


def best_plan(sizes):
    plans = [
        Plan(sizes, start, turn, flip)
        for start in range(sizes[2])
        for turn in (1, sizes[2] - 1)
        for flip in range(sizes[0])
    ]
    return min(plans, key=lambda plan: plan.price())


class Hop:
    def __init__(self, source, end, send_sem, recv_sem, site, here=None):
        self.parts = source, end, recv_sem
        self.copy = pltpu.make_async_remote_copy(
            src_ref=source,
            dst_ref=end,
            send_sem=send_sem,
            recv_sem=recv_sem,
            device_id=dict(zip(AXES, site)),
            device_id_type=pl.DeviceIdType.MESH,
        )
        self.away = None
        if here is not None:
            self.away = (site[0] != here[0]) | (site[1] != here[1]) | (site[2] != here[2])

    def start(self):
        if self.away is None:
            self.copy.start()
            return
        pl.when(self.away)(self.copy.start)
        pl.when(jnp.logical_not(self.away))(lambda: pltpu.make_async_copy(*self.parts).start())

    def wait_recv(self):
        self.copy.wait_recv()

    def wait_send(self):
        if self.away is None:
            self.copy.wait_send()
        else:
            pl.when(self.away)(self.copy.wait_send)


class Pick:
    def __init__(self, row, lane, count):
        self.lane = lane & (LANES - 1)
        self.masks = [row == r for r in range(count)]

    def __call__(self, table, start=0, init=None, stop=None):
        out = jnp.zeros(self.lane.shape, table.dtype) if init is None else init
        count = table.shape[0] if stop is None else stop
        for r in range(count):
            line = jnp.broadcast_to(table[r : r + 1, :], self.lane.shape)
            found = jnp.take_along_axis(line, self.lane, axis=1, mode="promise_in_bounds")
            out = jnp.where(self.masks[start + r], found, out)
        return out


def to_row(x):
    return jnp.concatenate([x[r : r + 1, :] for r in range(x.shape[0])], axis=1)


def to_rows(x):
    return jnp.concatenate(
        [x[:, LANES * r : LANES * (r + 1)] for r in range(x.shape[1] // LANES)], axis=0
    )


def one_hot_lanes(lane_row):
    shape = (LANES, lane_row.shape[1])
    hit = lax.broadcasted_iota(jnp.int32, shape, 0) == lane_row
    return jnp.where(hit, 1.0, 0.0).astype(jnp.bfloat16)


def place(row_row, values, hot, rows):
    shape = (rows, row_row.shape[1])
    hit = lax.broadcasted_iota(jnp.int32, shape, 0) == row_row
    left = jnp.concatenate([jnp.where(hit, v.astype(jnp.float32), 0.0) for v in values], axis=0)
    out = lax.dot_general(
        left.astype(jnp.bfloat16), hot, (((1,), (1,)), ((), ())), preferred_element_type=jnp.float32
    ).astype(jnp.int32)
    return [out[rows * i : rows * (i + 1)] for i in range(len(values))]


def kernel(plan, width, *refs):
    inputs, (move_ref, mult_ref) = refs[0:7], refs[7:9]
    (old_ref, new_ref, mass_ref, rest_ref, pairs_ref, live_ref, send_ref) = staged = refs[9:16]
    (listed, own_codes, codes, own_fields, fields_in, own_far, far_in, own_last, last_in,
     out_big, in_big, out_small, in_small, send_sem, recv_sem, carry_sem, load_sem) = refs[16:]
    rows = mass_ref.shape[0]
    slots = rows * LANES
    sizes = plan.sizes

    here = [lax.axis_index(axis) for axis in AXES]
    domain = plan.domain_on(here)
    homes_near = plan.around(domain)
    sites_near = [plan.site_of(d) for d in homes_near]
    sites_home_near = [plan.site_of(d) for d in plan.around(here)]
    greeted = [plan.site_of(here), domain] + sites_near + homes_near + sites_home_near
    barrier = pltpu.get_barrier_semaphore()
    for site in greeted:
        pl.semaphore_signal(
            barrier, inc=1, device_id=plan.named(site), device_id_type=pl.DeviceIdType.MESH
        )

    loads = [
        pltpu.make_async_copy(source, end, load_sem.at[i])
        for i, (source, end) in enumerate(zip(inputs, staged))
    ]
    for load in loads:
        load.start()

    slot_of, landings = [], []
    for n in sizes:
        base = len(landings)
        if n == 2:
            slot_of.append((base, base))
            landings.append(base)
        else:
            slot_of.append((base, base + 1))
            landings += [base, base + 1]
    started = []

    def go(hops):
        for hop in hops:
            hop.start()
        started.extend(hops)
        return hops

    def launch(number, tiles, sites, at=None):
        if number < 2:
            for i, tile in enumerate(tiles):
                out_big[number, i] = tile
        else:
            out_small[number - 2] = tiles[0]
        return go([
            Hop(
                out_big.at[number] if number < 2 else out_small.at[number - 2],
                in_big.at[number, landing] if number < 2 else in_small.at[number - 2, landing],
                send_sem.at[number, n],
                recv_sem.at[number, landing],
                site,
                at,
            )
            for n, (site, landing) in enumerate(zip(sites, landings))
        ])

    tile_row = lax.broadcasted_iota(jnp.int32, (8, LANES), 0)
    tile_lane = lax.broadcasted_iota(jnp.int32, (8, LANES), 1)
    back_half = tile_lane >= HALF

    def arrived(number, index=0, both_out=False):
        tiles = [
            in_big[number, n, index] if number < 2 else in_small[number - 2, n]
            for n in range(len(landings))
        ]
        out = tiles[slot_of[0][0]]
        for a in range(3):
            low, high = slot_of[a]
            if low == high:
                out = jnp.where(tile_row // 2 == a, tiles[low], out)
                continue
            odd = tile_row % 2 == 1
            from_up = odd if both_out else odd != back_half
            out = jnp.where(tile_row // 2 == a, jnp.where(from_up, tiles[high], tiles[low]), out)
        return out

    def wait(hops):
        for hop in hops:
            hop.wait_recv()

    for load in loads:
        load.wait()
    listed[...] = jnp.zeros_like(listed)
    listed[0:6, 0:width] = send_ref[...]
    listed[0:6, HALF : HALF + width] = send_ref[...]
    sending = listed[...]
    at_listed = Pick(sending >> 7, sending, rows)

    fields = [to_rows(ref[c : c + 1, :]) for ref in (old_ref, new_ref) for c in range(3)]
    fields = fields + [mass_ref[...]]
    for i, field in enumerate(fields + [rest_ref[...]]):
        own_fields[i] = field
    own_mass = fields[6]
    picked = [at_listed(f) for f in fields]
    picked.append(picked[6])
    tiles = [jnp.where(back_half, picked[2 * i + 1], picked[2 * i]) for i in range(BIG)]

    first = to_rows(pairs_ref[0:1, :])
    second = to_rows(pairs_ref[1:2, :])
    live = live_ref[...]
    own = second < slots
    offset = jnp.maximum(second - slots, 0)
    block = jnp.zeros_like(offset)
    for i in range(1, 6):
        block = block + jnp.where(offset >= width * i, 1, 0)
    second_row = jnp.where(own, second >> 7, rows + block)
    second_lane = jnp.where(own, second & (LANES - 1), offset - width * block)
    at_first = Pick(first >> 7, first, rows)
    at_second = Pick(second_row, second_lane, rows)
    number = (
        lax.broadcasted_iota(jnp.int32, (rows, LANES), 0) * LANES
        + lax.broadcasted_iota(jnp.int32, (rows, LANES), 1)
        + 1
    )
    counted = (live != 0) & (first != second)

    def code_row(mask_first, mask_second):
        return jnp.concatenate(
            [to_row(jnp.where(mask_first, first >> 7, -1)), to_row(jnp.where(mask_second, second_row, -1))], 1
        )

    hot = one_hot_lanes(jnp.concatenate([pairs_ref[0:1, :] & (LANES - 1), to_row(second_lane)], 1))
    number_row = to_row(number)
    number_row = jnp.concatenate([number_row, number_row + slots], 1)
    parts = [number_row >> 6, number_row & 63]
    high, low = place(code_row(counted, counted), parts, hot, rows + 8)
    ends = high * 64 + low
    ends_own = ends[:rows]
    ends_halo = ends[rows:]

    listed_row = jnp.concatenate([sending[b : b + 1, :] for b in range(6)], axis=1)
    spot = lax.broadcasted_iota(jnp.int32, listed_row.shape, 1)
    spot_lane = spot % LANES
    place_block, place_lane = place(
        jnp.where(spot_lane < width, listed_row >> 7, -1),
        [spot // LANES + 1, spot_lane],
        one_hot_lanes(listed_row & (LANES - 1)),
        rows,
    )

    minus_bit = (rows + 8) * LANES

    def coded(code):
        minus = code > slots
        index = jnp.where(minus, code - slots, code) - 1
        return jnp.where(code > 0, index + jnp.where(minus, minus_bit, 0), -1)

    def opened(code, count):
        minus = code >= minus_bit
        index = jnp.where(minus, code - minus_bit, code)
        return Pick(index >> 7, index, count), jnp.where(minus, -1.0, 1.0)

    other_first = jnp.where(counted, at_first(ends_own) - number, 0)
    other_second = jnp.where(counted & own, at_second(ends_own) - (number + slots), 0)
    far_code = jnp.where(place_block > 0, (place_block - 1) * LANES + HALF + place_lane, -1)
    reach = far_code + rows * LANES + 1
    reach = jnp.where(far_code >= 0, reach, 0)

    def partner(other, far):
        return jnp.where(other > 0, coded(other), far)

    second_code = second_row * LANES + second_lane
    lead_first = counted & ((other_first <= 0) | (number < other_first))
    lead_second = counted & own & ((other_second <= 0) | (number + slots < other_second))
    high, low = place(code_row(lead_first, lead_second), parts, hot, rows)
    lead = high * 64 + low
    send_code = jnp.where(back_half, pltpu.roll(ends_halo, HALF, 1), at_listed(ends_own))
    send_code = jnp.where(send_code > 2 * slots, 0, send_code)
    found = [
        live,
        first,
        second_code,
        partner(other_first, at_first(reach) - 1),
        partner(other_second, jnp.where(own, at_second(reach) - 1, second_code)),
        coded(send_code),
        coded(lead),
        coded(ends_own - lead),
        far_code,
    ]
    for i, code in enumerate(found):
        own_codes[i, 0 : code.shape[0]] = code

    pl.semaphore_wait(barrier, len(greeted))
    copies = launch(0, tiles, sites_home_near, here)

    def carry(index, source, end, site):
        return go([Hop(source, end, carry_sem.at[0, index], carry_sem.at[1, index], site, here)])

    inward = carry(0, own_codes, codes, greeted[0]) + carry(1, own_fields, fields_in, greeted[0])
    wait(inward)

    live, first, second_code = [codes[i, 0:rows] for i in range(3)]
    at_first = Pick(first >> 7, first, rows)
    at_second = Pick(second_code >> 7, second_code, rows + 6)
    along_first, sign_first = opened(codes[3, 0:rows], rows + 6)
    along_second, sign_second = opened(codes[4, 0:rows], rows + 6)
    to_send, send_sign = opened(codes[5, 0:8], rows)
    fields = [fields_in[i] for i in range(7)]
    mass, rest = fields[6], fields_in[7]
    near_first = [at_first(f) for f in fields]
    near_second = [at_second(f) for f in fields]

    wait(copies)
    got = [arrived(0, i, both_out=True) for i in range(BIG)]
    got_back = [pltpu.roll(t, HALF, 1) for t in got[:3]]
    halo = [got[0], got_back[0], got[1], got_back[1], got[2], got_back[2], got[3]]
    near_second = [at_second(h, rows, g, 6) for h, g in zip(halo, near_second)]
    mass_first, mass_second = near_first[6], near_second[6]
    old_span = [near_first[c] - near_second[c] for c in range(3)]
    new_span = [near_first[3 + c] - near_second[3 + c] for c in range(3)]
    dot = lambda p, q: p[0] * q[0] + p[1] * q[1] + p[2] * q[2]
    norm = jnp.sqrt(dot(old_span, old_span) + 0.25)
    unit = [s / norm for s in old_span]
    mass_sum = mass_first + mass_second
    scaling = live.astype(jnp.float32) / jnp.sqrt(mass_sum)
    weight = [scaling * u for u in unit]
    x = scaling * (dot(unit, new_span) - rest)

    copies = launch(1, [send_sign * to_send(w) for w in weight] + [to_send(x)], sites_near)
    at_lead, lead_sign = opened(codes[6, 0:rows], rows)
    at_rest, rest_sign = opened(codes[7, 0:rows], rows)
    at_far, unused = opened(codes[8, 0:rows], 6)
    diagonal = 1.0 - dot(weight, weight) * mass_sum
    pair_first = [along_first(w) for w in weight]
    pair_second = [along_second(w) for w in weight]
    lead_weight = [lead_sign * at_lead(w) for w in weight]
    rest_weight = [rest_sign * at_rest(w) for w in weight]
    near = along_first(x), along_second(x)
    wait(copies)
    got = [arrived(1, i) for i in range(BIG)]
    pair_first = [sign_first * along_first(h, rows, p, 6) for h, p in zip(got[:3], pair_first)]
    pair_second = [sign_second * along_second(h, rows, p, 6) for h, p in zip(got[:3], pair_second)]
    factor_first = -mass_first * dot(weight, pair_first)
    factor_second = mass_second * dot(weight, pair_second)
    halo_x = got[3]
    far_weight = None

    def finish(near, halo_x):
        return along_first(halo_x, rows, near[0], 6), along_second(halo_x, rows, near[1], 6)

    g = finish(near, halo_x)
    total_x, total_halo, total_g = x, halo_x, list(g)
    for index in range(2, ROUNDS):
        if index == 2 + ORDER:
            move_g = mass_first * total_g[0], mass_second * total_g[1]
            move_x = mass_sum * total_x
            stretch = [
                new_span[c] - move_x * weight[c] - move_g[0] * pair_first[c] + move_g[1] * pair_second[c]
                for c in range(3)
            ]
            length_sq = dot(stretch, stretch)
            target = jnp.sqrt(jnp.maximum(2.0 * rest * rest - length_sq, 0.25 * rest * rest))
            x = scaling * (rest - target)
        else:
            x = diagonal * x + factor_first * g[0] + factor_second * g[1]
        tile = [to_send(x)]
        if index == ROUNDS - 1:
            copies = launch(index, tile, homes_near, here)
            total_x = total_x + x
            break
        copies = launch(index, tile, sites_near)
        total_x = total_x + x
        near = along_first(x), along_second(x)
        if far_weight is None:
            far_weight = [-mass * at_far(h, stop=6) for h in got[:3]]
            for c in range(3):
                own_far[c] = far_weight[c]
            far_copy = carry(2, own_far, far_in, domain)
        wait(copies)
        halo_x = arrived(index)
        g = finish(near, halo_x)
        total_g = [t + h for t, h in zip(total_g, g)]
        total_halo = total_halo + halo_x

    at_ends = at_lead(total_x), at_rest(total_x), at_far(total_halo, stop=6)
    for c in range(3):
        own_last[c] = far_weight[c] * at_ends[2] - mass * (
            lead_weight[c] * at_ends[0] + rest_weight[c] * at_ends[1]
        )
    own_last[3] = total_x
    last_copy = carry(3, own_last, last_in, domain)
    at_far, unused = opened(far_code, 6)
    wait(far_copy)
    far_weight = [far_in[c] for c in range(3)]
    wait(copies)
    last = at_far(arrived(ROUNDS - 1), stop=6)
    wait(last_copy)
    mult_ref[...] = last_in[3]
    for c in range(3):
        move_ref[c : c + 1, :] = to_row(last_in[c] + far_weight[c] * last)
    for hop in started:
        hop.wait_send()


def solution(mesh):
    sizes = tuple(mesh.shape[a] for a in AXES)
    plan = best_plan(sizes)

    def per_device(old_pos, new_pos, inv_mass, rest_length, bond_pairs, live, send_index):
        atoms = old_pos.shape[1]
        rows = atoms // LANES
        width = send_index.shape[1]
        links = sum(1 if n == 2 else 2 for n in sizes)
        tall = lambda v: v.reshape(rows, LANES)
        vmem = pl.BlockSpec(memory_space=pltpu.VMEM)
        tile = (8, LANES)
        moved, mult = pl.pallas_call(
            functools.partial(kernel, plan, width),
            out_shape=(
                jax.ShapeDtypeStruct((3, atoms), jnp.float32),
                jax.ShapeDtypeStruct((rows, LANES), jnp.float32),
            ),
            in_specs=[pl.BlockSpec(memory_space=pl.ANY)] * 7,
            out_specs=(vmem, vmem),
            scratch_shapes=[
                pltpu.VMEM((3, atoms), jnp.float32),
                pltpu.VMEM((3, atoms), jnp.float32),
                pltpu.VMEM((rows, LANES), jnp.float32),
                pltpu.VMEM((rows, LANES), jnp.float32),
                pltpu.VMEM((2, atoms), jnp.int32),
                pltpu.VMEM((rows, LANES), jnp.int32),
                pltpu.VMEM(send_index.shape, jnp.int32),
                pltpu.VMEM(tile, jnp.int32),
                pltpu.VMEM((9, max(rows, 8), LANES), jnp.int32),
                pltpu.VMEM((9, max(rows, 8), LANES), jnp.int32),
                pltpu.VMEM((8, rows, LANES), jnp.float32),
                pltpu.VMEM((8, rows, LANES), jnp.float32),
                pltpu.VMEM((3, rows, LANES), jnp.float32),
                pltpu.VMEM((3, rows, LANES), jnp.float32),
                pltpu.VMEM((4, rows, LANES), jnp.float32),
                pltpu.VMEM((4, rows, LANES), jnp.float32),
                pltpu.VMEM((2, BIG) + tile, jnp.float32),
                pltpu.VMEM((2, links, BIG) + tile, jnp.float32),
                pltpu.VMEM((ROUNDS - 2,) + tile, jnp.float32),
                pltpu.VMEM((ROUNDS - 2, links) + tile, jnp.float32),
                pltpu.SemaphoreType.DMA((ROUNDS, links)),
                pltpu.SemaphoreType.DMA((ROUNDS, links)),
                pltpu.SemaphoreType.DMA((2, 4)),
                pltpu.SemaphoreType.DMA((7,)),
            ],
            compiler_params=pltpu.CompilerParams(collective_id=0, has_side_effects=True),
        )(old_pos, new_pos, tall(inv_mass), tall(rest_length), bond_pairs, tall(live), send_index)
        return moved, mult.reshape(atoms)

    spread = P(AXES)
    wide = P(None, AXES)
    return jax.shard_map(
        per_device,
        mesh=mesh,
        in_specs=(wide, wide, spread, spread, wide, spread, P(AXES, None)),
        out_specs=(wide, spread),
        check_vma=False,
    )
```

```python
import functools

import jax
import jax.numpy as jnp
from jax import lax
from jax.experimental import pallas as pl
from jax.experimental.pallas import tpu as pltpu
from jax.sharding import PartitionSpec as P

ORDER = 4
AXES = ("gx", "gy", "gz")
LANES = 128
HALF = 64
ROUNDS = 2 * ORDER + 3
BIG = 4


class Plan:
    def __init__(self, sizes, start, turn, flip):
        self.sizes, self.start, self.turn, self.flip = sizes, start, turn, flip

    def site_of(self, domain):
        ix, iy, iz = domain
        nx, ny, nz = self.sizes
        spot = (self.start + self.turn * iz) % nz
        if nz % 2 == 0:
            late = spot // (nz // 2)
            spot = (1 - late) * 2 * spot + late * (2 * (nz - 1 - spot) + 1)
        return [(ix + iy + iz + self.flip) % nx, iy, spot]

    def domain_on(self, site):
        core, iy, spot = site
        nx, ny, nz = self.sizes
        if nz % 2 == 0:
            line, side = spot // 2, spot % 2
            spot = (1 - side) * line + side * (nz - 1 - line)
        iz = (self.turn * (spot - self.start + nz) + nz) % nz
        return [(core + 2 * nx * (ny + nz) - iy - iz - self.flip) % nx, iy, iz]

    def named(self, site):
        return dict(zip(AXES, site))

    def around(self, domain):
        found = []
        for a, n in enumerate(self.sizes):
            for step in (1,) if n == 2 else (1, n - 1):
                found.append([(v + step) % n if i == a else v for i, v in enumerate(domain)])
        return found

    def price(self):
        worst = total = 0
        for ix in range(self.sizes[0]):
            for iy in range(self.sizes[1]):
                for iz in range(self.sizes[2]):
                    assert self.domain_on(self.site_of((ix, iy, iz))) == [ix, iy, iz]
                    for domain in [(ix, iy, iz)] + self.around((ix, iy, iz)):
                        site = self.site_of(domain)
                        hops = abs(site[2] // 2 - iz // 2) + abs(site[2] % 2 - iz % 2)
                        hops += abs(site[1] - iy)
                        worst, total = max(worst, hops), total + hops
        return worst, total


def best_plan(sizes):
    plans = [
        Plan(sizes, start, turn, flip)
        for start in range(sizes[2])
        for turn in (1, sizes[2] - 1)
        for flip in range(sizes[0])
    ]
    return min(plans, key=lambda plan: plan.price())


class Hop:
    def __init__(self, source, end, send_sem, recv_sem, site, here=None):
        self.parts = source, end, recv_sem
        self.copy = pltpu.make_async_remote_copy(
            src_ref=source,
            dst_ref=end,
            send_sem=send_sem,
            recv_sem=recv_sem,
            device_id=dict(zip(AXES, site)),
            device_id_type=pl.DeviceIdType.MESH,
        )
        self.away = None
        if here is not None:
            self.away = (site[0] != here[0]) | (site[1] != here[1]) | (site[2] != here[2])

    def start(self):
        if self.away is None:
            self.copy.start()
            return
        pl.when(self.away)(self.copy.start)
        pl.when(jnp.logical_not(self.away))(lambda: pltpu.make_async_copy(*self.parts).start())

    def wait_recv(self):
        self.copy.wait_recv()

    def wait_send(self):
        if self.away is None:
            self.copy.wait_send()
        else:
            pl.when(self.away)(self.copy.wait_send)


class Pick:
    def __init__(self, row, lane, count):
        self.lane = lane & (LANES - 1)
        self.masks = [row == r for r in range(count)]

    def __call__(self, table, start=0, init=None, stop=None):
        out = jnp.zeros(self.lane.shape, table.dtype) if init is None else init
        count = table.shape[0] if stop is None else stop
        for r in range(count):
            line = jnp.broadcast_to(table[r : r + 1, :], self.lane.shape)
            found = jnp.take_along_axis(line, self.lane, axis=1, mode="promise_in_bounds")
            out = jnp.where(self.masks[start + r], found, out)
        return out


def to_row(x):
    return jnp.concatenate([x[r : r + 1, :] for r in range(x.shape[0])], axis=1)


def to_rows(x):
    return jnp.concatenate(
        [x[:, LANES * r : LANES * (r + 1)] for r in range(x.shape[1] // LANES)], axis=0
    )


def one_hot_lanes(lane_row):
    shape = (LANES, lane_row.shape[1])
    hit = lax.broadcasted_iota(jnp.int32, shape, 0) == lane_row
    return jnp.where(hit, 1.0, 0.0).astype(jnp.bfloat16)


def place(row_row, values, hot, rows):
    shape = (rows, row_row.shape[1])
    hit = lax.broadcasted_iota(jnp.int32, shape, 0) == row_row
    left = jnp.concatenate([jnp.where(hit, v.astype(jnp.float32), 0.0) for v in values], axis=0)
    out = lax.dot_general(
        left.astype(jnp.bfloat16), hot, (((1,), (1,)), ((), ())), preferred_element_type=jnp.float32
    ).astype(jnp.int32)
    return [out[rows * i : rows * (i + 1)] for i in range(len(values))]


def kernel(plan, width, *refs):
    inputs, (move_ref, mult_ref) = refs[0:7], refs[7:9]
    (old_ref, new_ref, mass_ref, rest_ref, pairs_ref, live_ref, send_ref) = staged = refs[9:16]
    (listed, own_codes, codes, own_fields, fields_in, own_far, far_in, own_last, last_in,
     out_big, in_big, out_small, in_small, send_sem, recv_sem, carry_sem, load_sem) = refs[16:]
    rows = mass_ref.shape[0]
    slots = rows * LANES
    sizes = plan.sizes

    here = [lax.axis_index(axis) for axis in AXES]
    domain = plan.domain_on(here)
    homes_near = plan.around(domain)
    sites_near = [plan.site_of(d) for d in homes_near]
    sites_home_near = [plan.site_of(d) for d in plan.around(here)]
    greeted = [plan.site_of(here), domain] + sites_near + homes_near + sites_home_near
    barrier = pltpu.get_barrier_semaphore()
    for site in greeted:
        pl.semaphore_signal(
            barrier, inc=1, device_id=plan.named(site), device_id_type=pl.DeviceIdType.MESH
        )

    loads = [
        pltpu.make_async_copy(source, end, load_sem.at[i])
        for i, (source, end) in enumerate(zip(inputs, staged))
    ]
    for load in loads:
        load.start()

    slot_of, landings = [], []
    for n in sizes:
        base = len(landings)
        if n == 2:
            slot_of.append((base, base))
            landings.append(base)
        else:
            slot_of.append((base, base + 1))
            landings += [base, base + 1]
    started = []

    def go(hops):
        for hop in hops:
            hop.start()
        started.extend(hops)
        return hops

    def launch(number, tiles, sites, at=None):
        if number < 2:
            for i, tile in enumerate(tiles):
                out_big[number, i] = tile
        else:
            out_small[number - 2] = tiles[0]
        return go([
            Hop(
                out_big.at[number] if number < 2 else out_small.at[number - 2],
                in_big.at[number, landing] if number < 2 else in_small.at[number - 2, landing],
                send_sem.at[number, n],
                recv_sem.at[number, landing],
                site,
                at,
            )
            for n, (site, landing) in enumerate(zip(sites, landings))
        ])

    tile_row = lax.broadcasted_iota(jnp.int32, (8, LANES), 0)
    tile_lane = lax.broadcasted_iota(jnp.int32, (8, LANES), 1)
    back_half = tile_lane >= HALF

    def arrived(number, index=0, both_out=False):
        tiles = [
            in_big[number, n, index] if number < 2 else in_small[number - 2, n]
            for n in range(len(landings))
        ]
        out = tiles[slot_of[0][0]]
        for a in range(3):
            low, high = slot_of[a]
            if low == high:
                out = jnp.where(tile_row // 2 == a, tiles[low], out)
                continue
            odd = tile_row % 2 == 1
            from_up = odd if both_out else odd != back_half
            out = jnp.where(tile_row // 2 == a, jnp.where(from_up, tiles[high], tiles[low]), out)
        return out

    def wait(hops):
        for hop in hops:
            hop.wait_recv()

    for load in loads:
        load.wait()
    listed[...] = jnp.zeros_like(listed)
    listed[0:6, 0:width] = send_ref[...]
    listed[0:6, HALF : HALF + width] = send_ref[...]
    sending = listed[...]
    at_listed = Pick(sending >> 7, sending, rows)

    fields = [to_rows(ref[c : c + 1, :]) for ref in (old_ref, new_ref) for c in range(3)]
    fields = fields + [mass_ref[...]]
    for i, field in enumerate(fields + [rest_ref[...]]):
        own_fields[i] = field
    own_mass = fields[6]
    picked = [at_listed(f) for f in fields]
    picked.append(picked[6])
    tiles = [jnp.where(back_half, picked[2 * i + 1], picked[2 * i]) for i in range(BIG)]

    first = to_rows(pairs_ref[0:1, :])
    second = to_rows(pairs_ref[1:2, :])
    live = live_ref[...]
    own = second < slots
    offset = jnp.maximum(second - slots, 0)
    block = jnp.zeros_like(offset)
    for i in range(1, 6):
        block = block + jnp.where(offset >= width * i, 1, 0)
    second_row = jnp.where(own, second >> 7, rows + block)
    second_lane = jnp.where(own, second & (LANES - 1), offset - width * block)
    at_first = Pick(first >> 7, first, rows)
    at_second = Pick(second_row, second_lane, rows)
    number = (
        lax.broadcasted_iota(jnp.int32, (rows, LANES), 0) * LANES
        + lax.broadcasted_iota(jnp.int32, (rows, LANES), 1)
        + 1
    )
    counted = (live != 0) & (first != second)

    def code_row(mask_first, mask_second):
        return jnp.concatenate(
            [to_row(jnp.where(mask_first, first >> 7, -1)), to_row(jnp.where(mask_second, second_row, -1))], 1
        )

    hot = one_hot_lanes(jnp.concatenate([pairs_ref[0:1, :] & (LANES - 1), to_row(second_lane)], 1))
    number_row = to_row(number)
    number_row = jnp.concatenate([number_row, number_row + slots], 1)
    parts = [number_row >> 6, number_row & 63]
    high, low = place(code_row(counted, counted), parts, hot, rows + 8)
    ends = high * 64 + low
    ends_own = ends[:rows]
    ends_halo = ends[rows:]

    listed_row = jnp.concatenate([sending[b : b + 1, :] for b in range(6)], axis=1)
    spot = lax.broadcasted_iota(jnp.int32, listed_row.shape, 1)
    spot_lane = spot % LANES
    place_block, place_lane = place(
        jnp.where(spot_lane < width, listed_row >> 7, -1),
        [spot // LANES + 1, spot_lane],
        one_hot_lanes(listed_row & (LANES - 1)),
        rows,
    )

    minus_bit = (rows + 8) * LANES

    def coded(code):
        minus = code > slots
        index = jnp.where(minus, code - slots, code) - 1
        return jnp.where(code > 0, index + jnp.where(minus, minus_bit, 0), -1)

    def opened(code, count):
        minus = code >= minus_bit
        index = jnp.where(minus, code - minus_bit, code)
        return Pick(index >> 7, index, count), jnp.where(minus, -1.0, 1.0)

    other_first = jnp.where(counted, at_first(ends_own) - number, 0)
    other_second = jnp.where(counted & own, at_second(ends_own) - (number + slots), 0)
    far_code = jnp.where(place_block > 0, (place_block - 1) * LANES + HALF + place_lane, -1)
    reach = far_code + rows * LANES + 1
    reach = jnp.where(far_code >= 0, reach, 0)

    def partner(other, far):
        return jnp.where(other > 0, coded(other), far)

    second_code = second_row * LANES + second_lane
    lead_first = counted & ((other_first <= 0) | (number < other_first))
    lead_second = counted & own & ((other_second <= 0) | (number + slots < other_second))
    high, low = place(code_row(lead_first, lead_second), parts, hot, rows)
    lead = high * 64 + low
    send_code = jnp.where(back_half, pltpu.roll(ends_halo, HALF, 1), at_listed(ends_own))
    send_code = jnp.where(send_code > 2 * slots, 0, send_code)
    found = [
        live,
        first,
        second_code,
        partner(other_first, at_first(reach) - 1),
        partner(other_second, jnp.where(own, at_second(reach) - 1, second_code)),
        coded(send_code),
        coded(lead),
        coded(ends_own - lead),
        far_code,
    ]
    for i, code in enumerate(found):
        own_codes[i, 0 : code.shape[0]] = code

    pl.semaphore_wait(barrier, len(greeted))
    def carry(index, source, end, site):
        return go([Hop(source, end, carry_sem.at[0, index], carry_sem.at[1, index], site, here)])

    inward = carry(0, own_codes.at[0:6], codes.at[0:6], greeted[0])
    inward += carry(1, own_fields, fields_in, greeted[0])
    copies = launch(0, tiles, sites_home_near, here)
    later = carry(4, own_codes.at[6:9], codes.at[6:9], greeted[0])
    wait(inward)

    live, first, second_code = [codes[i, 0:rows] for i in range(3)]
    at_first = Pick(first >> 7, first, rows)
    at_second = Pick(second_code >> 7, second_code, rows + 6)
    along_first, sign_first = opened(codes[3, 0:rows], rows + 6)
    along_second, sign_second = opened(codes[4, 0:rows], rows + 6)
    to_send, send_sign = opened(codes[5, 0:8], rows)
    fields = [fields_in[i] for i in range(7)]
    mass, rest = fields[6], fields_in[7]
    near_first = [at_first(f) for f in fields]
    near_second = [at_second(f) for f in fields]

    wait(copies)
    got = [arrived(0, i, both_out=True) for i in range(BIG)]
    got_back = [pltpu.roll(t, HALF, 1) for t in got[:3]]
    halo = [got[0], got_back[0], got[1], got_back[1], got[2], got_back[2], got[3]]
    near_second = [at_second(h, rows, g, 6) for h, g in zip(halo, near_second)]
    mass_first, mass_second = near_first[6], near_second[6]
    old_span = [near_first[c] - near_second[c] for c in range(3)]
    new_span = [near_first[3 + c] - near_second[3 + c] for c in range(3)]
    dot = lambda p, q: p[0] * q[0] + p[1] * q[1] + p[2] * q[2]
    norm = jnp.sqrt(dot(old_span, old_span) + 0.25)
    unit = [s / norm for s in old_span]
    mass_sum = mass_first + mass_second
    scaling = live.astype(jnp.float32) / jnp.sqrt(mass_sum)
    weight = [scaling * u for u in unit]
    x = scaling * (dot(unit, new_span) - rest)

    copies = launch(1, [send_sign * to_send(w) for w in weight] + [to_send(x)], sites_near)
    wait(later)
    at_lead, lead_sign = opened(codes[6, 0:rows], rows)
    at_rest, rest_sign = opened(codes[7, 0:rows], rows)
    at_far, unused = opened(codes[8, 0:rows], 6)
    diagonal = 1.0 - dot(weight, weight) * mass_sum
    pair_first = [along_first(w) for w in weight]
    pair_second = [along_second(w) for w in weight]
    lead_weight = [lead_sign * at_lead(w) for w in weight]
    rest_weight = [rest_sign * at_rest(w) for w in weight]
    near = along_first(x), along_second(x)
    wait(copies)
    got = [arrived(1, i) for i in range(BIG)]
    pair_first = [sign_first * along_first(h, rows, p, 6) for h, p in zip(got[:3], pair_first)]
    pair_second = [sign_second * along_second(h, rows, p, 6) for h, p in zip(got[:3], pair_second)]
    factor_first = -mass_first * dot(weight, pair_first)
    factor_second = mass_second * dot(weight, pair_second)
    halo_x = got[3]
    far_weight = None

    def finish(near, halo_x):
        return along_first(halo_x, rows, near[0], 6), along_second(halo_x, rows, near[1], 6)

    g = finish(near, halo_x)
    total_x, total_halo, total_g = x, halo_x, list(g)
    for index in range(2, ROUNDS):
        if index == 2 + ORDER:
            move_g = mass_first * total_g[0], mass_second * total_g[1]
            move_x = mass_sum * total_x
            stretch = [
                new_span[c] - move_x * weight[c] - move_g[0] * pair_first[c] + move_g[1] * pair_second[c]
                for c in range(3)
            ]
            length_sq = dot(stretch, stretch)
            target = jnp.sqrt(jnp.maximum(2.0 * rest * rest - length_sq, 0.25 * rest * rest))
            x = scaling * (rest - target)
        else:
            x = diagonal * x + factor_first * g[0] + factor_second * g[1]
        tile = [to_send(x)]
        if index == ROUNDS - 1:
            copies = launch(index, tile, homes_near, here)
            total_x = total_x + x
            break
        copies = launch(index, tile, sites_near)
        total_x = total_x + x
        near = along_first(x), along_second(x)
        if far_weight is None:
            far_weight = [-mass * at_far(h, stop=6) for h in got[:3]]
            for c in range(3):
                own_far[c] = far_weight[c]
            far_copy = carry(2, own_far, far_in, domain)
        wait(copies)
        halo_x = arrived(index)
        g = finish(near, halo_x)
        total_g = [t + h for t, h in zip(total_g, g)]
        total_halo = total_halo + halo_x

    at_ends = at_lead(total_x), at_rest(total_x), at_far(total_halo, stop=6)
    for c in range(3):
        own_last[c] = far_weight[c] * at_ends[2] - mass * (
            lead_weight[c] * at_ends[0] + rest_weight[c] * at_ends[1]
        )
    own_last[3] = total_x
    last_copy = carry(3, own_last, last_in, domain)
    at_far, unused = opened(far_code, 6)
    wait(far_copy)
    far_weight = [far_in[c] for c in range(3)]
    wait(copies)
    last = at_far(arrived(ROUNDS - 1), stop=6)
    wait(last_copy)
    mult_ref[...] = last_in[3]
    for c in range(3):
        move_ref[c : c + 1, :] = to_row(last_in[c] + far_weight[c] * last)
    for hop in started:
        hop.wait_send()


def solution(mesh):
    sizes = tuple(mesh.shape[a] for a in AXES)
    plan = best_plan(sizes)

    def per_device(old_pos, new_pos, inv_mass, rest_length, bond_pairs, live, send_index):
        atoms = old_pos.shape[1]
        rows = atoms // LANES
        width = send_index.shape[1]
        links = sum(1 if n == 2 else 2 for n in sizes)
        tall = lambda v: v.reshape(rows, LANES)
        vmem = pl.BlockSpec(memory_space=pltpu.VMEM)
        tile = (8, LANES)
        moved, mult = pl.pallas_call(
            functools.partial(kernel, plan, width),
            out_shape=(
                pltpu.VMEM((3, atoms), jnp.float32),
                pltpu.VMEM((rows, LANES), jnp.float32),
            ),
            in_specs=[pl.BlockSpec(memory_space=pl.ANY)] * 7,
            out_specs=(vmem, vmem),
            scratch_shapes=[
                pltpu.VMEM((3, atoms), jnp.float32),
                pltpu.VMEM((3, atoms), jnp.float32),
                pltpu.VMEM((rows, LANES), jnp.float32),
                pltpu.VMEM((rows, LANES), jnp.float32),
                pltpu.VMEM((2, atoms), jnp.int32),
                pltpu.VMEM((rows, LANES), jnp.int32),
                pltpu.VMEM(send_index.shape, jnp.int32),
                pltpu.VMEM(tile, jnp.int32),
                pltpu.VMEM((9, max(rows, 8), LANES), jnp.int32),
                pltpu.VMEM((9, max(rows, 8), LANES), jnp.int32),
                pltpu.VMEM((8, rows, LANES), jnp.float32),
                pltpu.VMEM((8, rows, LANES), jnp.float32),
                pltpu.VMEM((3, rows, LANES), jnp.float32),
                pltpu.VMEM((3, rows, LANES), jnp.float32),
                pltpu.VMEM((4, rows, LANES), jnp.float32),
                pltpu.VMEM((4, rows, LANES), jnp.float32),
                pltpu.VMEM((2, BIG) + tile, jnp.float32),
                pltpu.VMEM((2, links, BIG) + tile, jnp.float32),
                pltpu.VMEM((ROUNDS - 2,) + tile, jnp.float32),
                pltpu.VMEM((ROUNDS - 2, links) + tile, jnp.float32),
                pltpu.SemaphoreType.DMA((ROUNDS, links)),
                pltpu.SemaphoreType.DMA((ROUNDS, links)),
                pltpu.SemaphoreType.DMA((2, 5)),
                pltpu.SemaphoreType.DMA((7,)),
            ],
            compiler_params=pltpu.CompilerParams(collective_id=0, has_side_effects=True),
        )(old_pos, new_pos, tall(inv_mass), tall(rest_length), bond_pairs, tall(live), send_index)
        return moved, mult.reshape(atoms)

    spread = P(AXES)
    wide = P(None, AXES)
    return jax.shard_map(
        per_device,
        mesh=mesh,
        in_specs=(wide, wide, spread, spread, wide, spread, P(AXES, None)),
        out_specs=(wide, spread),
        check_vma=False,
    )
```

```python
import functools

import jax
import jax.numpy as jnp
from jax import lax
from jax.experimental import pallas as pl
from jax.experimental.pallas import tpu as pltpu
from jax.sharding import PartitionSpec as P

ORDER = 4
AXES = ("gx", "gy", "gz")
LANES = 128
HALF = 64
ROUNDS = 2 * ORDER + 3
BIG = 4


class Plan:
    def __init__(self, sizes, start, turn, flip):
        self.sizes, self.start, self.turn, self.flip = sizes, start, turn, flip

    def site_of(self, domain):
        ix, iy, iz = domain
        nx, ny, nz = self.sizes
        spot = (self.start + self.turn * iz) % nz
        if nz % 2 == 0:
            late = spot // (nz // 2)
            spot = (1 - late) * 2 * spot + late * (2 * (nz - 1 - spot) + 1)
        return [(ix + iy + iz + self.flip) % nx, iy, spot]

    def domain_on(self, site):
        core, iy, spot = site
        nx, ny, nz = self.sizes
        if nz % 2 == 0:
            line, side = spot // 2, spot % 2
            spot = (1 - side) * line + side * (nz - 1 - line)
        iz = (self.turn * (spot - self.start + nz) + nz) % nz
        return [(core + 2 * nx * (ny + nz) - iy - iz - self.flip) % nx, iy, iz]

    def named(self, site):
        return dict(zip(AXES, site))

    def around(self, domain):
        found = []
        for a, n in enumerate(self.sizes):
            for step in (1,) if n == 2 else (1, n - 1):
                found.append([(v + step) % n if i == a else v for i, v in enumerate(domain)])
        return found

    def price(self):
        worst = total = 0
        for ix in range(self.sizes[0]):
            for iy in range(self.sizes[1]):
                for iz in range(self.sizes[2]):
                    assert self.domain_on(self.site_of((ix, iy, iz))) == [ix, iy, iz]
                    for domain in [(ix, iy, iz)] + self.around((ix, iy, iz)):
                        site = self.site_of(domain)
                        hops = abs(site[2] // 2 - iz // 2) + abs(site[2] % 2 - iz % 2)
                        hops += abs(site[1] - iy)
                        worst, total = max(worst, hops), total + hops
        return worst, total


def best_plan(sizes):
    plans = [
        Plan(sizes, start, turn, flip)
        for start in range(sizes[2])
        for turn in (1, sizes[2] - 1)
        for flip in range(sizes[0])
    ]
    return min(plans, key=lambda plan: plan.price())


class Hop:
    def __init__(self, source, end, send_sem, recv_sem, site, here=None):
        self.parts = source, end, recv_sem
        self.copy = pltpu.make_async_remote_copy(
            src_ref=source,
            dst_ref=end,
            send_sem=send_sem,
            recv_sem=recv_sem,
            device_id=dict(zip(AXES, site)),
            device_id_type=pl.DeviceIdType.MESH,
        )
        self.away = None
        if here is not None:
            self.away = (site[0] != here[0]) | (site[1] != here[1]) | (site[2] != here[2])

    def start(self):
        if self.away is None:
            self.copy.start()
            return
        pl.when(self.away)(self.copy.start)
        pl.when(jnp.logical_not(self.away))(lambda: pltpu.make_async_copy(*self.parts).start())

    def wait_recv(self):
        self.copy.wait_recv()

    def wait_send(self):
        if self.away is None:
            self.copy.wait_send()
        else:
            pl.when(self.away)(self.copy.wait_send)


class Pick:
    def __init__(self, row, lane, count):
        self.lane = lane & (LANES - 1)
        self.masks = [row == r for r in range(count)]

    def __call__(self, table, start=0, init=None, stop=None):
        if not isinstance(table, list):
            count = table.shape[0] if stop is None else stop
            table = [table[r : r + 1, :] for r in range(count)]
        out = jnp.zeros(self.lane.shape, table[0].dtype) if init is None else init
        for r, line in enumerate(table):
            line = jnp.broadcast_to(line, self.lane.shape)
            found = jnp.take_along_axis(line, self.lane, axis=1, mode="promise_in_bounds")
            out = jnp.where(self.masks[start + r], found, out)
        return out


def to_row(x):
    return jnp.concatenate([x[r : r + 1, :] for r in range(x.shape[0])], axis=1)


def to_rows(x):
    return jnp.concatenate(
        [x[:, LANES * r : LANES * (r + 1)] for r in range(x.shape[1] // LANES)], axis=0
    )


def one_hot_lanes(lane_row):
    shape = (LANES, lane_row.shape[1])
    hit = lax.broadcasted_iota(jnp.int32, shape, 0) == lane_row
    return jnp.where(hit, 1.0, 0.0).astype(jnp.bfloat16)


def place(row_row, values, hot, rows):
    shape = (rows, row_row.shape[1])
    hit = lax.broadcasted_iota(jnp.int32, shape, 0) == row_row
    left = jnp.concatenate([jnp.where(hit, v.astype(jnp.float32), 0.0) for v in values], axis=0)
    out = lax.dot_general(
        left.astype(jnp.bfloat16), hot, (((1,), (1,)), ((), ())), preferred_element_type=jnp.float32
    ).astype(jnp.int32)
    return [out[rows * i : rows * (i + 1)] for i in range(len(values))]


def kernel(plan, width, *refs):
    inputs, (move_ref, mult_ref) = refs[0:7], refs[7:9]
    (old_ref, new_ref, mass_ref, rest_ref, pairs_ref, live_ref, send_ref) = staged = refs[9:16]
    (listed, own_codes, codes, own_fields, fields_in, own_far, far_in, own_last, last_in,
     out_big, in_big, out_small, in_small, send_sem, recv_sem, carry_sem, load_sem) = refs[16:]
    rows = mass_ref.shape[0]
    slots = rows * LANES
    sizes = plan.sizes

    here = [lax.axis_index(axis) for axis in AXES]
    domain = plan.domain_on(here)
    homes_near = plan.around(domain)
    sites_near = [plan.site_of(d) for d in homes_near]
    sites_home_near = [plan.site_of(d) for d in plan.around(here)]
    greeted = [plan.site_of(here), domain] + sites_near + homes_near + sites_home_near
    barrier = pltpu.get_barrier_semaphore()
    for site in greeted:
        pl.semaphore_signal(
            barrier, inc=1, device_id=plan.named(site), device_id_type=pl.DeviceIdType.MESH
        )

    loads = [
        pltpu.make_async_copy(source, end, load_sem.at[i])
        for i, (source, end) in enumerate(zip(inputs, staged))
    ]
    for load in loads:
        load.start()

    slot_of, landings, axis_of = [], [], []
    for a, n in enumerate(sizes):
        base = len(landings)
        if n == 2:
            slot_of.append((base, base))
            landings.append(base)
            axis_of.append(a)
        else:
            slot_of.append((base, base + 1))
            landings += [base, base + 1]
            axis_of += [a, a]
    started = []

    def go(hops):
        for hop in hops:
            hop.start()
        started.extend(hops)
        return hops

    def launch(number, tiles, sites, at=None):
        if number < 2:
            for a in range(3):
                out_big[number, a] = jnp.concatenate([t[2 * a : 2 * a + 2] for t in tiles], axis=0)
        else:
            out_small[number - 2] = tiles[0]
        return go([
            Hop(
                out_big.at[number, axis_of[n]] if number < 2 else out_small.at[number - 2],
                in_big.at[number, landing] if number < 2 else in_small.at[number - 2, landing],
                send_sem.at[number, n],
                recv_sem.at[number, landing],
                site,
                at,
            )
            for n, (site, landing) in enumerate(zip(sites, landings))
        ])

    tile_row = lax.broadcasted_iota(jnp.int32, (8, LANES), 0)
    tile_lane = lax.broadcasted_iota(jnp.int32, (8, LANES), 1)
    back_half = tile_lane >= HALF

    def merged(tiles, a):
        low, high = slot_of[a]
        if low == high:
            return tiles[low]
        return jnp.where((tile_row % 2 == 1) != back_half, tiles[high], tiles[low])

    def arrived(number):
        tiles = [in_small[number - 2, n] for n in range(len(landings))]
        out = merged(tiles, 0)
        for a in range(1, 3):
            out = jnp.where(tile_row // 2 == a, merged(tiles, a), out)
        return out

    def wait(hops):
        for hop in hops:
            hop.wait_recv()

    for load in loads:
        load.wait()
    listed[...] = jnp.zeros_like(listed)
    listed[0:6, 0:width] = send_ref[...]
    listed[0:6, HALF : HALF + width] = send_ref[...]
    sending = listed[...]
    at_listed = Pick(sending >> 7, sending, rows)

    fields = [to_rows(ref[c : c + 1, :]) for ref in (old_ref, new_ref) for c in range(3)]
    fields = fields + [mass_ref[...]]
    for i, field in enumerate(fields + [rest_ref[...]]):
        own_fields[i] = field
    own_mass = fields[6]
    picked = [at_listed(f) for f in fields]
    picked.append(picked[6])
    tiles = [jnp.where(back_half, picked[2 * i + 1], picked[2 * i]) for i in range(BIG)]

    first = to_rows(pairs_ref[0:1, :])
    second = to_rows(pairs_ref[1:2, :])
    live = live_ref[...]
    own = second < slots
    offset = jnp.maximum(second - slots, 0)
    block = jnp.zeros_like(offset)
    for i in range(1, 6):
        block = block + jnp.where(offset >= width * i, 1, 0)
    second_row = jnp.where(own, second >> 7, rows + block)
    second_lane = jnp.where(own, second & (LANES - 1), offset - width * block)
    at_first = Pick(first >> 7, first, rows)
    at_second = Pick(second_row, second_lane, rows)
    number = (
        lax.broadcasted_iota(jnp.int32, (rows, LANES), 0) * LANES
        + lax.broadcasted_iota(jnp.int32, (rows, LANES), 1)
        + 1
    )
    counted = (live != 0) & (first != second)

    def code_row(mask_first, mask_second):
        return jnp.concatenate(
            [to_row(jnp.where(mask_first, first >> 7, -1)), to_row(jnp.where(mask_second, second_row, -1))], 1
        )

    hot = one_hot_lanes(jnp.concatenate([pairs_ref[0:1, :] & (LANES - 1), to_row(second_lane)], 1))
    number_row = to_row(number)
    number_row = jnp.concatenate([number_row, number_row + slots], 1)
    parts = [number_row >> 6, number_row & 63]
    high, low = place(code_row(counted, counted), parts, hot, rows + 8)
    ends = high * 64 + low
    ends_own = ends[:rows]
    ends_halo = ends[rows:]

    listed_row = jnp.concatenate([sending[b : b + 1, :] for b in range(6)], axis=1)
    spot = lax.broadcasted_iota(jnp.int32, listed_row.shape, 1)
    spot_lane = spot % LANES
    place_block, place_lane = place(
        jnp.where(spot_lane < width, listed_row >> 7, -1),
        [spot // LANES + 1, spot_lane],
        one_hot_lanes(listed_row & (LANES - 1)),
        rows,
    )

    minus_bit = (rows + 8) * LANES

    def coded(code):
        minus = code > slots
        index = jnp.where(minus, code - slots, code) - 1
        return jnp.where(code > 0, index + jnp.where(minus, minus_bit, 0), -1)

    def opened(code, count):
        minus = code >= minus_bit
        index = jnp.where(minus, code - minus_bit, code)
        return Pick(index >> 7, index, count), jnp.where(minus, -1.0, 1.0)

    other_first = jnp.where(counted, at_first(ends_own) - number, 0)
    other_second = jnp.where(counted & own, at_second(ends_own) - (number + slots), 0)
    far_code = jnp.where(place_block > 0, (place_block - 1) * LANES + HALF + place_lane, -1)
    reach = far_code + rows * LANES + 1
    reach = jnp.where(far_code >= 0, reach, 0)

    def partner(other, far):
        return jnp.where(other > 0, coded(other), far)

    second_code = second_row * LANES + second_lane
    lead_first = counted & ((other_first <= 0) | (number < other_first))
    lead_second = counted & own & ((other_second <= 0) | (number + slots < other_second))
    high, low = place(code_row(lead_first, lead_second), parts, hot, rows)
    lead = high * 64 + low
    send_code = jnp.where(back_half, pltpu.roll(ends_halo, HALF, 1), at_listed(ends_own))
    send_code = jnp.where(send_code > 2 * slots, 0, send_code)
    found = [
        live,
        first,
        second_code,
        partner(other_first, at_first(reach) - 1),
        partner(other_second, jnp.where(own, at_second(reach) - 1, second_code)),
        coded(send_code),
        coded(lead),
        coded(ends_own - lead),
        far_code,
    ]
    for i, code in enumerate(found):
        own_codes[i, 0 : code.shape[0]] = code

    pl.semaphore_wait(barrier, len(greeted))
    def carry(index, source, end, site):
        return go([Hop(source, end, carry_sem.at[0, index], carry_sem.at[1, index], site, here)])

    inward = carry(0, own_codes.at[0:6], codes.at[0:6], greeted[0])
    inward += carry(1, own_fields, fields_in, greeted[0])
    copies = launch(0, tiles, sites_home_near, here)
    later = carry(4, own_codes.at[6:9], codes.at[6:9], greeted[0])
    wait(inward)

    live, first, second_code = [codes[i, 0:rows] for i in range(3)]
    at_first = Pick(first >> 7, first, rows)
    at_second = Pick(second_code >> 7, second_code, rows + 6)
    along_first, sign_first = opened(codes[3, 0:rows], rows + 6)
    along_second, sign_second = opened(codes[4, 0:rows], rows + 6)
    to_send, send_sign = opened(codes[5, 0:8], rows)
    fields = [fields_in[i] for i in range(7)]
    mass, rest = fields[6], fields_in[7]
    near_first = [at_first(f) for f in fields]
    near_second = [at_second(f) for f in fields]

    wait(copies)
    tiles = [in_big[0, n] for n in range(len(landings))]
    turned = [pltpu.roll(t, HALF, 1) for t in tiles]
    halo = []
    for i in range(7):
        source, t = (turned if i % 2 else tiles), i // 2
        halo.append([
            source[slot_of[a][side]][2 * t + side : 2 * t + side + 1]
            for a in range(3)
            for side in range(2)
        ])
    near_second = [at_second(h, rows, g, 6) for h, g in zip(halo, near_second)]
    mass_first, mass_second = near_first[6], near_second[6]
    old_span = [near_first[c] - near_second[c] for c in range(3)]
    new_span = [near_first[3 + c] - near_second[3 + c] for c in range(3)]
    dot = lambda p, q: p[0] * q[0] + p[1] * q[1] + p[2] * q[2]
    norm = jnp.sqrt(dot(old_span, old_span) + 0.25)
    unit = [s / norm for s in old_span]
    mass_sum = mass_first + mass_second
    scaling = live.astype(jnp.float32) / jnp.sqrt(mass_sum)
    weight = [scaling * u for u in unit]
    x = scaling * (dot(unit, new_span) - rest)

    copies = launch(1, [send_sign * to_send(w) for w in weight] + [to_send(x)], sites_near)
    wait(later)
    at_lead, lead_sign = opened(codes[6, 0:rows], rows)
    at_rest, rest_sign = opened(codes[7, 0:rows], rows)
    at_far, unused = opened(codes[8, 0:rows], 6)
    diagonal = 1.0 - dot(weight, weight) * mass_sum
    pair_first = [along_first(w) for w in weight]
    pair_second = [along_second(w) for w in weight]
    lead_weight = [lead_sign * at_lead(w) for w in weight]
    rest_weight = [rest_sign * at_rest(w) for w in weight]
    near = along_first(x), along_second(x)
    wait(copies)
    tiles = [in_big[1, n] for n in range(len(landings))]
    tiles = [merged(tiles, a) for a in range(3)]
    got = [
        [tiles[a][2 * t + side : 2 * t + side + 1] for a in range(3) for side in range(2)]
        for t in range(BIG - 1)
    ]
    halo_x = jnp.concatenate(
        [t[2 * BIG - 2 : 2 * BIG] for t in tiles] + [jnp.zeros((2, LANES), jnp.float32)], axis=0
    )
    pair_first = [sign_first * along_first(h, rows, p, 6) for h, p in zip(got[:3], pair_first)]
    pair_second = [sign_second * along_second(h, rows, p, 6) for h, p in zip(got[:3], pair_second)]
    factor_first = -mass_first * dot(weight, pair_first)
    factor_second = mass_second * dot(weight, pair_second)
    far_weight = None

    def finish(near, halo_x):
        return along_first(halo_x, rows, near[0], 6), along_second(halo_x, rows, near[1], 6)

    g = finish(near, halo_x)
    total_x, total_halo, total_g = x, halo_x, list(g)
    for index in range(2, ROUNDS):
        if index == 2 + ORDER:
            move_g = mass_first * total_g[0], mass_second * total_g[1]
            move_x = mass_sum * total_x
            stretch = [
                new_span[c] - move_x * weight[c] - move_g[0] * pair_first[c] + move_g[1] * pair_second[c]
                for c in range(3)
            ]
            length_sq = dot(stretch, stretch)
            target = jnp.sqrt(jnp.maximum(2.0 * rest * rest - length_sq, 0.25 * rest * rest))
            x = scaling * (rest - target)
        else:
            x = diagonal * x + factor_first * g[0] + factor_second * g[1]
        tile = [to_send(x)]
        if index == ROUNDS - 1:
            copies = launch(index, tile, homes_near, here)
            total_x = total_x + x
            break
        copies = launch(index, tile, sites_near)
        total_x = total_x + x
        near = along_first(x), along_second(x)
        if far_weight is None:
            far_weight = [-mass * at_far(h, stop=6) for h in got[:3]]
            for c in range(3):
                own_far[c] = far_weight[c]
            far_copy = carry(2, own_far, far_in, domain)
        wait(copies)
        halo_x = arrived(index)
        g = finish(near, halo_x)
        total_g = [t + h for t, h in zip(total_g, g)]
        total_halo = total_halo + halo_x

    at_ends = at_lead(total_x), at_rest(total_x), at_far(total_halo, stop=6)
    for c in range(3):
        own_last[c] = far_weight[c] * at_ends[2] - mass * (
            lead_weight[c] * at_ends[0] + rest_weight[c] * at_ends[1]
        )
    own_last[3] = total_x
    last_copy = carry(3, own_last, last_in, domain)
    at_far, unused = opened(far_code, 6)
    wait(far_copy)
    far_weight = [far_in[c] for c in range(3)]
    wait(copies)
    last = at_far(arrived(ROUNDS - 1), stop=6)
    wait(last_copy)
    mult_ref[...] = last_in[3]
    for c in range(3):
        move_ref[c : c + 1, :] = to_row(last_in[c] + far_weight[c] * last)
    for hop in started:
        hop.wait_send()


def solution(mesh):
    sizes = tuple(mesh.shape[a] for a in AXES)
    plan = best_plan(sizes)

    def per_device(old_pos, new_pos, inv_mass, rest_length, bond_pairs, live, send_index):
        atoms = old_pos.shape[1]
        rows = atoms // LANES
        width = send_index.shape[1]
        links = sum(1 if n == 2 else 2 for n in sizes)
        tall = lambda v: v.reshape(rows, LANES)
        vmem = pl.BlockSpec(memory_space=pltpu.VMEM)
        tile = (8, LANES)
        moved, mult = pl.pallas_call(
            functools.partial(kernel, plan, width),
            out_shape=(
                pltpu.VMEM((3, atoms), jnp.float32),
                pltpu.VMEM((rows, LANES), jnp.float32),
            ),
            in_specs=[pl.BlockSpec(memory_space=pl.ANY)] * 7,
            out_specs=(vmem, vmem),
            scratch_shapes=[
                pltpu.VMEM((3, atoms), jnp.float32),
                pltpu.VMEM((3, atoms), jnp.float32),
                pltpu.VMEM((rows, LANES), jnp.float32),
                pltpu.VMEM((rows, LANES), jnp.float32),
                pltpu.VMEM((2, atoms), jnp.int32),
                pltpu.VMEM((rows, LANES), jnp.int32),
                pltpu.VMEM(send_index.shape, jnp.int32),
                pltpu.VMEM(tile, jnp.int32),
                pltpu.VMEM((9, max(rows, 8), LANES), jnp.int32),
                pltpu.VMEM((9, max(rows, 8), LANES), jnp.int32),
                pltpu.VMEM((8, rows, LANES), jnp.float32),
                pltpu.VMEM((8, rows, LANES), jnp.float32),
                pltpu.VMEM((3, rows, LANES), jnp.float32),
                pltpu.VMEM((3, rows, LANES), jnp.float32),
                pltpu.VMEM((4, rows, LANES), jnp.float32),
                pltpu.VMEM((4, rows, LANES), jnp.float32),
                pltpu.VMEM((2, 3) + tile, jnp.float32),
                pltpu.VMEM((2, links) + tile, jnp.float32),
                pltpu.VMEM((ROUNDS - 2,) + tile, jnp.float32),
                pltpu.VMEM((ROUNDS - 2, links) + tile, jnp.float32),
                pltpu.SemaphoreType.DMA((ROUNDS, links)),
                pltpu.SemaphoreType.DMA((ROUNDS, links)),
                pltpu.SemaphoreType.DMA((2, 5)),
                pltpu.SemaphoreType.DMA((7,)),
            ],
            compiler_params=pltpu.CompilerParams(collective_id=0, has_side_effects=True),
        )(old_pos, new_pos, tall(inv_mass), tall(rest_length), bond_pairs, tall(live), send_index)
        return moved, mult.reshape(atoms)

    spread = P(AXES)
    wide = P(None, AXES)
    return jax.shard_map(
        per_device,
        mesh=mesh,
        in_specs=(wide, wide, spread, spread, wide, spread, P(AXES, None)),
        out_specs=(wide, spread),
        check_vma=False,
    )
```

```python
import functools

import jax
import jax.numpy as jnp
from jax import lax
from jax.experimental import pallas as pl
from jax.experimental.pallas import tpu as pltpu
from jax.sharding import PartitionSpec as P

ORDER = 4
AXES = ("gx", "gy", "gz")
LANES = 128
HALF = 64
ROUNDS = 2 * ORDER + 3
BIG = 4


class Plan:
    def __init__(self, sizes, start, turn, flip):
        self.sizes, self.start, self.turn, self.flip = sizes, start, turn, flip

    def site_of(self, domain):
        ix, iy, iz = domain
        nx, ny, nz = self.sizes
        spot = (self.start + self.turn * iz) % nz
        if nz % 2 == 0:
            late = spot // (nz // 2)
            spot = (1 - late) * 2 * spot + late * (2 * (nz - 1 - spot) + 1)
        return [(ix + iy + iz + self.flip) % nx, iy, spot]

    def domain_on(self, site):
        core, iy, spot = site
        nx, ny, nz = self.sizes
        if nz % 2 == 0:
            line, side = spot // 2, spot % 2
            spot = (1 - side) * line + side * (nz - 1 - line)
        iz = (self.turn * (spot - self.start + nz) + nz) % nz
        return [(core + 2 * nx * (ny + nz) - iy - iz - self.flip) % nx, iy, iz]

    def named(self, site):
        return dict(zip(AXES, site))

    def around(self, domain):
        found = []
        for a, n in enumerate(self.sizes):
            for step in (1,) if n == 2 else (1, n - 1):
                found.append([(v + step) % n if i == a else v for i, v in enumerate(domain)])
        return found

    def price(self):
        worst = total = 0
        for ix in range(self.sizes[0]):
            for iy in range(self.sizes[1]):
                for iz in range(self.sizes[2]):
                    assert self.domain_on(self.site_of((ix, iy, iz))) == [ix, iy, iz]
                    for domain in [(ix, iy, iz)] + self.around((ix, iy, iz)):
                        site = self.site_of(domain)
                        hops = abs(site[2] // 2 - iz // 2) + abs(site[2] % 2 - iz % 2)
                        hops += abs(site[1] - iy)
                        worst, total = max(worst, hops), total + hops
        return worst, total


def best_plan(sizes):
    plans = [
        Plan(sizes, start, turn, flip)
        for start in range(sizes[2])
        for turn in (1, sizes[2] - 1)
        for flip in range(sizes[0])
    ]
    return min(plans, key=lambda plan: plan.price())


class Hop:
    def __init__(self, source, end, send_sem, recv_sem, site, here=None):
        self.parts = source, end, recv_sem
        self.copy = pltpu.make_async_remote_copy(
            src_ref=source,
            dst_ref=end,
            send_sem=send_sem,
            recv_sem=recv_sem,
            device_id=dict(zip(AXES, site)),
            device_id_type=pl.DeviceIdType.MESH,
        )
        self.away = None
        if here is not None:
            self.away = (site[0] != here[0]) | (site[1] != here[1]) | (site[2] != here[2])

    def start(self):
        if self.away is None:
            self.copy.start()
            return
        pl.when(self.away)(self.copy.start)
        pl.when(jnp.logical_not(self.away))(lambda: pltpu.make_async_copy(*self.parts).start())

    def wait_recv(self):
        self.copy.wait_recv()

    def wait_send(self):
        if self.away is None:
            self.copy.wait_send()
        else:
            pl.when(self.away)(self.copy.wait_send)


class Pick:
    def __init__(self, row, lane, count):
        self.lane = lane & (LANES - 1)
        self.masks = [row == r for r in range(count)]

    def __call__(self, table, start=0, init=None, stop=None):
        if not isinstance(table, list):
            count = table.shape[0] if stop is None else stop
            table = [table[r : r + 1, :] for r in range(count)]
        out = jnp.zeros(self.lane.shape, table[0].dtype) if init is None else init
        for r, line in enumerate(table):
            line = jnp.broadcast_to(line, self.lane.shape)
            found = jnp.take_along_axis(line, self.lane, axis=1, mode="promise_in_bounds")
            out = jnp.where(self.masks[start + r], found, out)
        return out


def to_row(x):
    return jnp.concatenate([x[r : r + 1, :] for r in range(x.shape[0])], axis=1)


def to_rows(x):
    return jnp.concatenate(
        [x[:, LANES * r : LANES * (r + 1)] for r in range(x.shape[1] // LANES)], axis=0
    )


def one_hot_lanes(lane_row):
    shape = (LANES, lane_row.shape[1])
    hit = lax.broadcasted_iota(jnp.int32, shape, 0) == lane_row
    return jnp.where(hit, 1.0, 0.0).astype(jnp.bfloat16)


def place(row_row, values, hot, rows):
    shape = (rows, row_row.shape[1])
    hit = lax.broadcasted_iota(jnp.int32, shape, 0) == row_row
    left = jnp.concatenate([jnp.where(hit, v.astype(jnp.float32), 0.0) for v in values], axis=0)
    out = lax.dot_general(
        left.astype(jnp.bfloat16), hot, (((1,), (1,)), ((), ())), preferred_element_type=jnp.float32
    ).astype(jnp.int32)
    return [out[rows * i : rows * (i + 1)] for i in range(len(values))]


def kernel(plan, width, *refs):
    inputs, (move_ref, mult_ref) = refs[0:7], refs[7:9]
    (old_ref, new_ref, mass_ref, rest_ref, pairs_ref, live_ref, send_ref) = staged = refs[9:16]
    (listed, own_codes, codes, own_fields, fields_in, own_far, far_in, own_last, last_in,
     out_big, in_big, out_small, in_small, send_sem, recv_sem, carry_sem, load_sem) = refs[16:]
    rows = mass_ref.shape[0]
    slots = rows * LANES
    sizes = plan.sizes

    here = [lax.axis_index(axis) for axis in AXES]
    domain = plan.domain_on(here)
    homes_near = plan.around(domain)
    sites_near = [plan.site_of(d) for d in homes_near]
    sites_home_near = [plan.site_of(d) for d in plan.around(here)]
    greeted = [plan.site_of(here), domain] + sites_near + homes_near + sites_home_near
    barrier = pltpu.get_barrier_semaphore()
    for site in greeted:
        pl.semaphore_signal(
            barrier, inc=1, device_id=plan.named(site), device_id_type=pl.DeviceIdType.MESH
        )

    loads = [
        pltpu.make_async_copy(source, end, load_sem.at[i])
        for i, (source, end) in enumerate(zip(inputs, staged))
    ]
    for load in loads:
        load.start()

    slot_of, landings, axis_of = [], [], []
    for a, n in enumerate(sizes):
        base = len(landings)
        if n == 2:
            slot_of.append((base, base))
            landings.append(base)
            axis_of.append(a)
        else:
            slot_of.append((base, base + 1))
            landings += [base, base + 1]
            axis_of += [a, a]
    started = []

    def go(hops):
        for hop in hops:
            hop.start()
        started.extend(hops)
        return hops

    def launch(number, tiles, sites, at=None):
        if number < 2:
            for a in range(3):
                out_big[number, a] = jnp.concatenate([t[2 * a : 2 * a + 2] for t in tiles], axis=0)
        else:
            for a in range(3):
                out_small[number - 2, a] = tiles[0][2 * a : 2 * a + 2]
        return go([
            Hop(
                out_big.at[number, axis_of[n]] if number < 2 else out_small.at[number - 2, axis_of[n]],
                in_big.at[number, landing] if number < 2 else in_small.at[number - 2, landing],
                send_sem.at[number, n],
                recv_sem.at[number, landing],
                site,
                at,
            )
            for n, (site, landing) in enumerate(zip(sites, landings))
        ])

    tile_row = lax.broadcasted_iota(jnp.int32, (8, LANES), 0)
    tile_lane = lax.broadcasted_iota(jnp.int32, (8, LANES), 1)
    back_half = tile_lane >= HALF

    upper = (tile_row % 2 == 1) != back_half

    def merged(tiles, a):
        low, high = slot_of[a]
        if low == high:
            return tiles[low]
        return jnp.where(upper[: tiles[low].shape[0]], tiles[high], tiles[low])

    def arrived(number):
        tiles = [in_small[number - 2, n] for n in range(len(landings))]
        return [merged(tiles, a) for a in range(3)]

    def lines(pairs):
        return [pair[side : side + 1] for pair in pairs for side in range(2)]

    def wait(hops):
        for hop in hops:
            hop.wait_recv()

    for load in loads:
        load.wait()
    listed[...] = jnp.zeros_like(listed)
    listed[0:6, 0:width] = send_ref[...]
    listed[0:6, HALF : HALF + width] = send_ref[...]
    sending = listed[...]
    at_listed = Pick(sending >> 7, sending, rows)

    fields = [to_rows(ref[c : c + 1, :]) for ref in (old_ref, new_ref) for c in range(3)]
    fields = fields + [mass_ref[...]]
    for i, field in enumerate(fields + [rest_ref[...]]):
        own_fields[i] = field
    own_mass = fields[6]
    picked = [at_listed(f) for f in fields]
    picked.append(picked[6])
    tiles = [jnp.where(back_half, picked[2 * i + 1], picked[2 * i]) for i in range(BIG)]

    first = to_rows(pairs_ref[0:1, :])
    second = to_rows(pairs_ref[1:2, :])
    live = live_ref[...]
    own = second < slots
    offset = jnp.maximum(second - slots, 0)
    block = jnp.zeros_like(offset)
    for i in range(1, 6):
        block = block + jnp.where(offset >= width * i, 1, 0)
    second_row = jnp.where(own, second >> 7, rows + block)
    second_lane = jnp.where(own, second & (LANES - 1), offset - width * block)
    at_first = Pick(first >> 7, first, rows)
    at_second = Pick(second_row, second_lane, rows)
    number = (
        lax.broadcasted_iota(jnp.int32, (rows, LANES), 0) * LANES
        + lax.broadcasted_iota(jnp.int32, (rows, LANES), 1)
        + 1
    )
    counted = (live != 0) & (first != second)

    def code_row(mask_first, mask_second):
        return jnp.concatenate(
            [to_row(jnp.where(mask_first, first >> 7, -1)), to_row(jnp.where(mask_second, second_row, -1))], 1
        )

    hot = one_hot_lanes(jnp.concatenate([pairs_ref[0:1, :] & (LANES - 1), to_row(second_lane)], 1))
    number_row = to_row(number)
    number_row = jnp.concatenate([number_row, number_row + slots], 1)
    parts = [number_row >> 6, number_row & 63]
    high, low = place(code_row(counted, counted), parts, hot, rows + 8)
    ends = high * 64 + low
    ends_own = ends[:rows]
    ends_halo = ends[rows:]

    listed_row = jnp.concatenate([sending[b : b + 1, :] for b in range(6)], axis=1)
    spot = lax.broadcasted_iota(jnp.int32, listed_row.shape, 1)
    spot_lane = spot % LANES
    place_block, place_lane = place(
        jnp.where(spot_lane < width, listed_row >> 7, -1),
        [spot // LANES + 1, spot_lane],
        one_hot_lanes(listed_row & (LANES - 1)),
        rows,
    )

    minus_bit = (rows + 8) * LANES

    def coded(code):
        minus = code > slots
        index = jnp.where(minus, code - slots, code) - 1
        return jnp.where(code > 0, index + jnp.where(minus, minus_bit, 0), -1)

    def opened(code, count):
        minus = code >= minus_bit
        index = jnp.where(minus, code - minus_bit, code)
        return Pick(index >> 7, index, count), jnp.where(minus, -1.0, 1.0)

    other_first = jnp.where(counted, at_first(ends_own) - number, 0)
    other_second = jnp.where(counted & own, at_second(ends_own) - (number + slots), 0)
    far_code = jnp.where(place_block > 0, (place_block - 1) * LANES + HALF + place_lane, -1)
    reach = far_code + rows * LANES + 1
    reach = jnp.where(far_code >= 0, reach, 0)

    def partner(other, far):
        return jnp.where(other > 0, coded(other), far)

    second_code = second_row * LANES + second_lane
    lead_first = counted & ((other_first <= 0) | (number < other_first))
    lead_second = counted & own & ((other_second <= 0) | (number + slots < other_second))
    high, low = place(code_row(lead_first, lead_second), parts, hot, rows)
    lead = high * 64 + low
    send_code = jnp.where(back_half, pltpu.roll(ends_halo, HALF, 1), at_listed(ends_own))
    send_code = jnp.where(send_code > 2 * slots, 0, send_code)
    found = [
        live,
        first,
        second_code,
        partner(other_first, at_first(reach) - 1),
        partner(other_second, jnp.where(own, at_second(reach) - 1, second_code)),
        coded(send_code),
        coded(lead),
        coded(ends_own - lead),
        far_code,
    ]
    for i, code in enumerate(found):
        own_codes[i, 0 : code.shape[0]] = code

    pl.semaphore_wait(barrier, len(greeted))
    def carry(index, source, end, site):
        return go([Hop(source, end, carry_sem.at[0, index], carry_sem.at[1, index], site, here)])

    inward = carry(0, own_codes.at[0:6], codes.at[0:6], greeted[0])
    inward += carry(1, own_fields, fields_in, greeted[0])
    copies = launch(0, tiles, sites_home_near, here)
    later = carry(4, own_codes.at[6:9], codes.at[6:9], greeted[0])
    wait(inward)

    live, first, second_code = [codes[i, 0:rows] for i in range(3)]
    at_first = Pick(first >> 7, first, rows)
    at_second = Pick(second_code >> 7, second_code, rows + 6)
    along_first, sign_first = opened(codes[3, 0:rows], rows + 6)
    along_second, sign_second = opened(codes[4, 0:rows], rows + 6)
    to_send, send_sign = opened(codes[5, 0:8], rows)
    fields = [fields_in[i] for i in range(7)]
    mass, rest = fields[6], fields_in[7]
    near_first = [at_first(f) for f in fields]
    near_second = [at_second(f) for f in fields]

    wait(copies)
    tiles = [in_big[0, n] for n in range(len(landings))]
    turned = [pltpu.roll(t, HALF, 1) for t in tiles]
    halo = []
    for i in range(7):
        source, t = (turned if i % 2 else tiles), i // 2
        halo.append([
            source[slot_of[a][side]][2 * t + side : 2 * t + side + 1]
            for a in range(3)
            for side in range(2)
        ])
    near_second = [at_second(h, rows, g, 6) for h, g in zip(halo, near_second)]
    mass_first, mass_second = near_first[6], near_second[6]
    old_span = [near_first[c] - near_second[c] for c in range(3)]
    new_span = [near_first[3 + c] - near_second[3 + c] for c in range(3)]
    dot = lambda p, q: p[0] * q[0] + p[1] * q[1] + p[2] * q[2]
    norm = jnp.sqrt(dot(old_span, old_span) + 0.25)
    unit = [s / norm for s in old_span]
    mass_sum = mass_first + mass_second
    scaling = live.astype(jnp.float32) / jnp.sqrt(mass_sum)
    weight = [scaling * u for u in unit]
    x = scaling * (dot(unit, new_span) - rest)

    copies = launch(1, [send_sign * to_send(w) for w in weight] + [to_send(x)], sites_near)
    wait(later)
    at_lead, lead_sign = opened(codes[6, 0:rows], rows)
    at_rest, rest_sign = opened(codes[7, 0:rows], rows)
    at_far, unused = opened(codes[8, 0:rows], 6)
    diagonal = 1.0 - dot(weight, weight) * mass_sum
    pair_first = [along_first(w) for w in weight]
    pair_second = [along_second(w) for w in weight]
    lead_weight = [lead_sign * at_lead(w) for w in weight]
    rest_weight = [rest_sign * at_rest(w) for w in weight]
    near = along_first(x), along_second(x)
    wait(copies)
    tiles = [in_big[1, n] for n in range(len(landings))]
    tiles = [merged(tiles, a) for a in range(3)]
    got = [
        [tiles[a][2 * t + side : 2 * t + side + 1] for a in range(3) for side in range(2)]
        for t in range(BIG - 1)
    ]
    halo_x = [t[2 * BIG - 2 : 2 * BIG] for t in tiles]
    pair_first = [sign_first * along_first(h, rows, p, 6) for h, p in zip(got[:3], pair_first)]
    pair_second = [sign_second * along_second(h, rows, p, 6) for h, p in zip(got[:3], pair_second)]
    factor_first = -mass_first * dot(weight, pair_first)
    factor_second = mass_second * dot(weight, pair_second)
    far_weight = None

    def finish(near, halo_x):
        halo_x = lines(halo_x)
        return along_first(halo_x, rows, near[0]), along_second(halo_x, rows, near[1])

    g = finish(near, halo_x)
    total_x, total_halo, total_g = x, halo_x, list(g)
    for index in range(2, ROUNDS):
        if index == 2 + ORDER:
            move_g = mass_first * total_g[0], mass_second * total_g[1]
            move_x = mass_sum * total_x
            stretch = [
                new_span[c] - move_x * weight[c] - move_g[0] * pair_first[c] + move_g[1] * pair_second[c]
                for c in range(3)
            ]
            length_sq = dot(stretch, stretch)
            target = jnp.sqrt(jnp.maximum(2.0 * rest * rest - length_sq, 0.25 * rest * rest))
            x = scaling * (rest - target)
        else:
            x = diagonal * x + factor_first * g[0] + factor_second * g[1]
        tile = [to_send(x)]
        if index == ROUNDS - 1:
            copies = launch(index, tile, homes_near, here)
            total_x = total_x + x
            break
        copies = launch(index, tile, sites_near)
        total_x = total_x + x
        near = along_first(x), along_second(x)
        if far_weight is None:
            far_weight = [-mass * at_far(h, stop=6) for h in got[:3]]
            for c in range(3):
                own_far[c] = far_weight[c]
            far_copy = carry(2, own_far, far_in, domain)
        wait(copies)
        halo_x = arrived(index)
        g = finish(near, halo_x)
        total_g = [t + h for t, h in zip(total_g, g)]
        total_halo = [t + h for t, h in zip(total_halo, halo_x)]

    at_ends = at_lead(total_x), at_rest(total_x), at_far(lines(total_halo))
    for c in range(3):
        own_last[c] = far_weight[c] * at_ends[2] - mass * (
            lead_weight[c] * at_ends[0] + rest_weight[c] * at_ends[1]
        )
    own_last[3] = total_x
    last_copy = carry(3, own_last, last_in, domain)
    at_far, unused = opened(far_code, 6)
    wait(far_copy)
    far_weight = [far_in[c] for c in range(3)]
    wait(copies)
    last = at_far(lines(arrived(ROUNDS - 1)))
    wait(last_copy)
    mult_ref[...] = last_in[3]
    for c in range(3):
        move_ref[c : c + 1, :] = to_row(last_in[c] + far_weight[c] * last)
    for hop in started:
        hop.wait_send()


def solution(mesh):
    sizes = tuple(mesh.shape[a] for a in AXES)
    plan = best_plan(sizes)

    def per_device(old_pos, new_pos, inv_mass, rest_length, bond_pairs, live, send_index):
        atoms = old_pos.shape[1]
        rows = atoms // LANES
        width = send_index.shape[1]
        links = sum(1 if n == 2 else 2 for n in sizes)
        tall = lambda v: v.reshape(rows, LANES)
        vmem = pl.BlockSpec(memory_space=pltpu.VMEM)
        tile = (8, LANES)
        moved, mult = pl.pallas_call(
            functools.partial(kernel, plan, width),
            out_shape=(
                pltpu.VMEM((3, atoms), jnp.float32),
                pltpu.VMEM((rows, LANES), jnp.float32),
            ),
            in_specs=[pl.BlockSpec(memory_space=pl.ANY)] * 7,
            out_specs=(vmem, vmem),
            scratch_shapes=[
                pltpu.VMEM((3, atoms), jnp.float32),
                pltpu.VMEM((3, atoms), jnp.float32),
                pltpu.VMEM((rows, LANES), jnp.float32),
                pltpu.VMEM((rows, LANES), jnp.float32),
                pltpu.VMEM((2, atoms), jnp.int32),
                pltpu.VMEM((rows, LANES), jnp.int32),
                pltpu.VMEM(send_index.shape, jnp.int32),
                pltpu.VMEM(tile, jnp.int32),
                pltpu.VMEM((9, max(rows, 8), LANES), jnp.int32),
                pltpu.VMEM((9, max(rows, 8), LANES), jnp.int32),
                pltpu.VMEM((8, rows, LANES), jnp.float32),
                pltpu.VMEM((8, rows, LANES), jnp.float32),
                pltpu.VMEM((3, rows, LANES), jnp.float32),
                pltpu.VMEM((3, rows, LANES), jnp.float32),
                pltpu.VMEM((4, rows, LANES), jnp.float32),
                pltpu.VMEM((4, rows, LANES), jnp.float32),
                pltpu.VMEM((2, 3) + tile, jnp.float32),
                pltpu.VMEM((2, links) + tile, jnp.float32),
                pltpu.VMEM((ROUNDS - 2, 3, 2, LANES), jnp.float32),
                pltpu.VMEM((ROUNDS - 2, links, 2, LANES), jnp.float32),
                pltpu.SemaphoreType.DMA((ROUNDS, links)),
                pltpu.SemaphoreType.DMA((ROUNDS, links)),
                pltpu.SemaphoreType.DMA((2, 5)),
                pltpu.SemaphoreType.DMA((7,)),
            ],
            compiler_params=pltpu.CompilerParams(collective_id=0, has_side_effects=True),
        )(old_pos, new_pos, tall(inv_mass), tall(rest_length), bond_pairs, tall(live), send_index)
        return moved, mult.reshape(atoms)

    spread = P(AXES)
    wide = P(None, AXES)
    return jax.shard_map(
        per_device,
        mesh=mesh,
        in_specs=(wide, wide, spread, spread, wide, spread, P(AXES, None)),
        out_specs=(wide, spread),
        check_vma=False,
    )
```
